32 devices in a mesh: dp: 16 (over z, y, core), tensor: 2 (over x).
Axes of the slice: x: 2, y: 2, z: 4, core: 2. Of those that a mesh axis runs over, the one named last changes fastest.
Arguments:
- activations: bfloat16 [24576, 2048], P('dp', 'tensor'), may hold values from -6 to 6
- out_grads: bfloat16 [24576, 2048], P('dp', 'tensor'), may hold values from -0.00390625 to 0.00390625
- left_stat: float32 [2048, 2048], P('dp', 'tensor'), may hold values from -1 to 11, as said below
- right_stat: float32 [2048, 2048], P('dp', 'tensor'), may hold values from -1 to 11, as said below
Outputs:
- left_new: float32 [2048, 2048], P('dp', 'tensor')
- right_new: float32 [2048, 2048], P('dp', 'tensor')
- update: float32 [2048, 2048], P('dp', 'tensor')
The draws below stay inside these ranges and needn't reach their ends.
Inputs may be any that keep to these rules, and one draw needn't show every extreme that they name: `left_stat`: symmetric, with a positive diagonal. `right_stat`: symmetric, with a positive diagonal.
All inputs are finite; a program needn't handle non-finite values.
Results may differ from the reference program's by a relative error of at most 0.0012.
Values may be sent and summed in bfloat16 or wider, within the bound.
No kernel may reach another device: no remote copies, remote signals or barrier semaphores. Data moves between devices by JAX's collectives and lax.ppermute only.
A program may use at most 64 MiB of HBM per device.

```python
import math
import jax
import jax.numpy as jnp
from jax import lax

B = 2048
TOKENS = 24576


def stat_matrix(key):
    first_key, second_key = jax.random.split(key)
    noise = jax.random.normal(first_key, (B, B), jnp.float32)
    symmetric = (noise + noise.T) * (0.3 / math.sqrt(2 * B))
    diagonal = jnp.exp(jax.random.uniform(second_key, (B,), jnp.float32, math.log(0.25), math.log(4.0)))
    return symmetric + jnp.diag(diagonal)


def draw_left_stat(key, part):
    return stat_matrix(jax.random.fold_in(key, 11))


def draw_right_stat(key, part):
    return stat_matrix(jax.random.fold_in(key, 23))


def steps_of(own_key, dims, shards, least, largest):
    factor_of, own = 1.0, jax.random.fold_in(own_key, 6)
    for dim, blocks in shards:
        heights = jnp.exp(jax.random.uniform(jax.random.fold_in(own, dim), (blocks,), jnp.float32, least / len(shards), largest / len(shards)))
        factor_of = factor_of * jnp.repeat(heights, dims[dim] // blocks).reshape([-1 if axis == dim else 1 for axis in range(len(dims))])
    return factor_of


def scatter_about(stream_key, extent, deviation, most, cuts=(), dtype=jnp.bfloat16):
    drawn = deviation * jax.random.normal(stream_key, extent, jnp.float32)
    if cuts:
        drawn = drawn * steps_of(stream_key, extent, cuts, -0.22, 0.18)
    return jnp.clip(drawn, -most, most).astype(dtype)


def setup_inputs(seed: int = 0) -> dict:
    streams_of = jax.random.split(jax.random.key(seed), 5)
    activations = scatter_about(streams_of[0], (TOKENS, B), 1.0, 6.0, ((0, 16), (1, 2)))
    out_grads = scatter_about(streams_of[1], (TOKENS, B), (2 * (TOKENS * B) ** -0.5), 0.00390625, ((0, 16), (1, 2)))
    left_stat = draw_left_stat(jax.random.fold_in(streams_of[4], 71), 0)
    right_stat = draw_right_stat(jax.random.fold_in(streams_of[4], 71), 0)
    return dict(activations=activations, out_grads=out_grads, left_stat=left_stat, right_stat=right_stat)


def reference(activations, out_grads, left_stat, right_stat):
    highest = lax.Precision.HIGHEST
    gradient = lax.dot_general(activations, out_grads, (((0,), (0,)), ((), ())), preferred_element_type=jnp.float32)
    left_new = 0.9 * left_stat + 0.1 * jnp.dot(gradient, gradient.T, precision=highest, preferred_element_type=jnp.float32)
    right_new = 0.9 * right_stat + 0.1 * jnp.dot(gradient.T, gradient, precision=highest, preferred_element_type=jnp.float32)
    left_scale = jnp.sqrt(jnp.sum(left_new * left_new) / B + 1e-06)
    right_scale = jnp.sqrt(jnp.sum(right_new * right_new) / B + 1e-06)
    pre_left = 5.0 * gradient - jnp.dot(left_new, gradient, precision=highest, preferred_element_type=jnp.float32) / left_scale
    pre = 5.0 * pre_left - jnp.dot(pre_left, right_new, precision=highest, preferred_element_type=jnp.float32) / right_scale
    factor = jnp.sqrt(jnp.sum(gradient * gradient) + 1e-06) / jnp.sqrt(jnp.sum(pre * pre) + 1e-06)
    return (left_new, right_new, pre * factor)
```

```python
import functools

import jax
import jax.numpy as jnp
from jax import lax
from jax.experimental import pallas as pl
from jax.experimental.pallas import tpu as pltpu
from jax.sharding import PartitionSpec as P

BF16, F32 = jnp.bfloat16, jnp.float32


def swap(x, axis, mask, sources=None):
    count = lax.axis_size(axis)
    pairs = [(i, i ^ mask) for i in range(count) if sources is None or sources(i)]
    return lax.ppermute(x, axis, pairs)


def dot(a, b, left, right):
    return lax.dot_general(a, b, (((left,), (right,)), ((), ())), preferred_element_type=F32)


def split(x):
    high = lax.reduce_precision(x, 8, 7)
    return high.astype(BF16), (x - high).astype(BF16)


def join(mine, other, bit, axis):
    first = jnp.where(bit == 0, mine, other)
    second = jnp.where(bit == 0, other, mine)
    return jnp.stack([first, second], axis)


def products(runs, count, scalars, left_rows, positions, right_rows, right_stat, grad_parts, grad_block, arrays):
    rows, cols = grad_block.shape
    order = right_rows.shape[0]
    tile = min(cols, 256)

    def kernel(s_ref, left_ref, pos_ref, right_ref, stat_ref, grad_ref, *rest):
        grow_refs, rest = rest[: count - 1], rest[count - 1 :]
        refs, rest = rest[: len(arrays)], rest[len(arrays) :]
        left_out, right_out, x_out, y_out, z_out, sums_out, lnew, lsplit, xfull, turn, lhs = rest

        def load(run, s, span):
            index, blocks, part = run[2][s]
            return refs[index][s, blocks, part, span].reshape(run[1], -1)

        every = slice(0, cols)
        grad = grad_ref[...]
        grad_high = grad.astype(BF16)
        grad_low = (grad - grad_high.astype(F32)).astype(BF16)
        lhs[:rows, :cols] = grad_high
        for s in range(1, count):
            lhs[:rows, s * cols : (s + 1) * cols] = grow_refs[s - 1][...]
        both = jnp.concatenate([grad_high, grad_low], 0)
        for run in runs:
            value = dot(both, load(run, 0, every), 1, 1)
            value = value[:rows] + value[rows:]
            for s in range(1, count):
                value += dot(grow_refs[s - 1][...], load(run, s, every), 1, 1)
            span = slice(run[0], run[0] + run[1])
            turn[:rows, span] = value.astype(BF16)
            new = 0.9 * left_ref[:, span] + 0.1 * value
            lnew[:, span] = new
            high = new.astype(BF16)
            lsplit[:rows, span] = high
            lsplit[rows:, span] = (new - high.astype(F32)).astype(BF16)
        left_out[...] = lnew[:, :cols]
        spot = s_ref[0] + lax.broadcasted_iota(jnp.int32, (rows, order), 0)
        diagonal = jnp.sum(jnp.where(pos_ref[0:1, :] == spot, lnew[...], 0.0), 1, keepdims=True)
        for s in range(count):
            for n in range(0, cols, tile):
                value = None
                for run in runs:
                    term = dot(lsplit[:, run[0] : run[0] + run[1]], load(run, s, slice(n, n + tile)), 1, 0)
                    value = term if value is None else value + term
                value = value[:rows] + value[rows:]
                if s == 0:
                    value += diagonal * grad_low[:, n : n + tile].astype(F32)
                    x_out[:, n : n + tile] = value
                high = value.astype(BF16)
                span = slice(s * cols + n, s * cols + n + tile)
                lhs[rows : 2 * rows, span] = high
                lhs[2 * rows :, span] = (value - high.astype(F32)).astype(BF16)
        for run in runs:
            value = None
            for s in range(count):
                term = dot(lhs[rows : 2 * rows, s * cols : (s + 1) * cols], load(run, s, every), 1, 1)
                value = term if value is None else value + term
            turn[rows:, run[0] : run[0] + run[1]] = value.astype(BF16)
        strips = []
        for run in runs:
            strip = None
            for s in range(count):
                if rows % 128 == 0:
                    part = load(run, s, pl.ds(pl.multiple_of(s_ref[2], 128), rows))
                else:
                    wide = (cols, rows)
                    pick = lax.broadcasted_iota(jnp.int32, wide, 0) == s_ref[2] + lax.broadcasted_iota(jnp.int32, wide, 1)
                    part = dot(load(run, s, every), pick.astype(F32).astype(BF16), 1, 0).astype(BF16)
                keep = (s_ref[1] == s).astype(F32).astype(BF16)
                strip = part * keep if strip is None else strip + part * keep
            strips.append(strip)
        for n in range(0, cols, tile):
            span = slice(n, n + tile)
            stat = dot(lhs[...], right_ref[:, span], 1, 0)
            stat_low = dot(grad_low, right_ref[:cols, span], 1, 0)
            moved, gram = None, None
            for run, strip in zip(runs, strips):
                base = load(run, 0, span)
                term = dot(turn[:, run[0] : run[0] + run[1]], base, 1, 0)
                moved = term if moved is None else moved + term
                term = dot(strip, base, 0, 0)
                gram = term if gram is None else gram + term
            y_out[:, span] = 0.9 * (stat[:rows] + stat_low) + 0.1 * moved[:rows]
            z_out[:, span] = 0.9 * (stat[rows : 2 * rows] + stat[2 * rows :]) + 0.1 * moved[rows:]
            right_out[:, span] = 0.9 * stat_ref[:, span] + 0.1 * gram
        terms = (grad, x_out[...], y_out[...], z_out[...])
        left, right = left_out[...], right_out[...]
        values = [left * left, right * right] + [terms[i] * terms[j] for i in range(4) for j in range(i, 4)]
        lane = lax.broadcasted_iota(jnp.int32, (8, 128), 1)
        total = jnp.zeros((8, 128), F32)
        for k, value in enumerate(values):
            total = jnp.where(lane == k, jnp.sum(value), total)
        sums_out[...] = total

    vmem = pl.BlockSpec(memory_space=pltpu.VMEM)
    block = jax.ShapeDtypeStruct((rows, cols), F32)
    flops = 2 * rows * order * (2 * order + 2 * order + order + 5 * cols)
    return pl.pallas_call(
        kernel,
        out_shape=(block,) * 5 + (jax.ShapeDtypeStruct((8, 128), F32),),
        in_specs=[pl.BlockSpec(memory_space=pltpu.SMEM)] + [vmem] * (4 + count + len(arrays)),
        out_specs=(vmem,) * 6,
        scratch_shapes=[
            pltpu.VMEM((rows, order), F32),
            pltpu.VMEM((2 * rows, order), BF16),
            pltpu.VMEM((8, 128), BF16),
            pltpu.VMEM((2 * rows, order), BF16),
            pltpu.VMEM((3 * rows, order), BF16),
        ],
        compiler_params=pltpu.CompilerParams(vmem_limit_bytes=48 * 1024 * 1024),
        cost_estimate=pl.CostEstimate(flops=flops, bytes_accessed=16 * order * cols, transcendentals=0),
        name="products",
    )(scalars, left_rows, positions, right_rows, right_stat, grad_block, *grad_parts, *arrays)


def finish(order, mine, other, grad, x, y, z):
    rows, cols = grad.shape

    def kernel(a_ref, b_ref, g_ref, x_ref, y_ref, z_ref, out_ref):
        total = a_ref[...] + b_ref[...]
        lane = lax.broadcasted_iota(jnp.int32, total.shape, 1)

        def value(k):
            return jnp.sum(jnp.where(lane == k, total, 0.0), 1, keepdims=True)[0:1]

        left = 1.0 / jnp.sqrt(value(0) / order + 1e-06)
        right = 1.0 / jnp.sqrt(value(1) / order + 1e-06)
        weights = (jnp.full_like(left, 25.0), -5.0 * left, -5.0 * right, left * right)
        pairs = [(i, j) for i in range(4) for j in range(i, 4)]
        norm = 1e-06
        for k, (i, j) in enumerate(pairs):
            norm = norm + (1.0 if i == j else 2.0) * weights[i] * weights[j] * value(2 + k)
        factor = jnp.sqrt(value(2) + 1e-06) / jnp.sqrt(jnp.maximum(norm, 1e-06))
        c0, c1, c2, c3 = [w * factor for w in weights]
        out_ref[...] = c0 * g_ref[...] + c1 * x_ref[...] + c2 * y_ref[...] + c3 * z_ref[...]

    return pl.pallas_call(
        kernel,
        out_shape=jax.ShapeDtypeStruct((rows, cols), F32),
        cost_estimate=pl.CostEstimate(flops=8 * rows * cols, bytes_accessed=20 * rows * cols, transcendentals=0),
        name="finish",
    )(mine, other, grad, x, y, z)


def local(activations, out_grads, left_stat, right_stat):
    count = lax.axis_size("tensor")
    dp_count = lax.axis_size("dp")
    tensor_bits = count.bit_length() - 1
    dp_bits = dp_count.bit_length() - 1
    low_bits = dp_bits - tensor_bits
    low = 1 << low_bits
    tokens, cols = out_grads.shape
    order = cols * count
    rows = order // dp_count
    place = lax.axis_index("dp")
    side = lax.axis_index("tensor")
    bit = [(place >> b) & 1 for b in range(dp_bits)]
    low_place = place & (low - 1)
    own = (place >> low_bits) ^ side
    top = low_bits - 1
    half = low // 2
    token = [None]

    def event(function, *inputs):
        if token[0] is not None:
            inputs, _ = lax.optimization_barrier((inputs, token[0]))
        out = function(*inputs)
        token[0] = out
        return out

    if rows % 64 == 0:
        cuts = [(0, 0, rows), (1, 0, rows // 2), (1, rows // 2, rows)]
    else:
        cuts = [(0, 0, rows), (1, 0, rows)]

    def cut(array, group, start, stop):
        part = array[:, group * half * rows : (group + 1) * half * rows]
        if stop - start == rows:
            return part
        return part.reshape(tokens, half, rows)[:, :, start:stop].reshape(tokens, half * (stop - start))

    def send_features(k):
        piece = event(lambda a: cut(a, *cuts[k]), activations)
        return [None] + [swap(piece, "tensor", r) for r in range(1, count)]

    def halves(total, b, axis):
        keep = lax.dynamic_index_in_dim(total, bit[b], axis, keepdims=False)
        return keep, lax.dynamic_index_in_dim(total, 1 - bit[b], axis, keepdims=False)

    def begin(features, width, bits):
        def step(f, o):
            return halves(dot(f, o, 0, 0).reshape((2,) * bits + (width, cols)), 0, bits - 1)

        keep, send = event(step, features, out_grads)
        return keep, swap(send, "dp", 1)

    def reduce_next(state, b, axis):
        keep, send = event(lambda k, r: halves(k + r, b, axis), *state)
        return keep, swap(send, "dp", 1 << b)

    def reduce_whole(state, mask, sources=None):
        total = event(lambda k, r: k + r, *state)
        return total, swap(total, "dp", mask, sources)

    def at_group(group):
        return lambda i: ((i >> top) & 1) == group

    def off_group(group):
        return lambda i: ((i >> top) & 1) != group

    def spread_first(state, group):
        def step(k, r):
            total = k + r
            return total, total.astype(BF16)

        total, high = event(step, *state)
        if group is None:
            return total, (high, swap(high, "dp", 1 << top))
        return total, (high, swap(high, "dp", 1 << top, at_group(group)))

    def spread_second(pair, group):
        def step(mine, other):
            held = join(mine, other, bit[top], 0) if group is None else jnp.where(bit[top] == group, mine, other)[None]
            return held[..., : cols // 2], held[..., cols // 2 :]

        ahead, behind = event(step, *pair)
        return (ahead, swap(ahead, "dp", 2)), (behind, [swap(behind, "tensor", s) for s in range(1, count)])

    def spread_third(first, second):
        def step(mine, other, held, others):
            return join(mine, other, bit[1], 1), jnp.stack([held] + others)

        ahead, behind = event(step, *first, *second)
        return (ahead, [swap(ahead, "tensor", s) for s in range(1, count)]), (behind, swap(behind, "dp", 2))

    def spread_fourth(first, second):
        def step(held, others, mine, other):
            return jnp.concatenate([jnp.stack([held] + others), join(mine, other, bit[1], 2)], -1)

        held = event(step, *first, *second)
        return held, swap(held, "dp", 1)

    arrivals = [send_features(0)]
    right_held = event(lambda r: r.astype(BF16), right_stat)
    right_other = swap(right_held, "dp", 2)
    arrivals += [send_features(k) for k in range(1, len(cuts))]
    left_parts = [left_stat] + [swap(left_stat, "tensor", s) for s in range(1, count)]

    def right_order(b):
        return bit[b] ^ ((side >> (b - low_bits)) & 1) if b >= low_bits else bit[b]

    state = begin(activations, rows, low_bits)
    right_held = event(lambda m, o: join(m, o, bit[1], 0), right_held, right_other)
    right_bits = [b for b in range(dp_bits - 1, 1, -1)]
    right_other = swap(right_held, "dp", 1 << right_bits[0])
    state = reduce_next(state, 1, low_bits - 2)
    for place_of, b in enumerate(right_bits):
        right_held = event(lambda m, o: join(m, o, right_order(b), place_of), right_held, right_other)
        following = right_bits[place_of + 1] if place_of + 1 < len(right_bits) else 0
        right_other = swap(right_held, "dp", 1 << following)

    remote = {}
    for r in range(1, count):
        for k, (group, start, stop) in enumerate(cuts):
            remote[r, k] = None

    keys = [(r, k) for k in range(len(cuts)) for r in range(1, count)]

    def begin_remote(key):
        r, k = key
        group, start, stop = cuts[k]
        remote[key] = begin(arrivals[k][r], stop - start, low_bits - 1)

    def next_remote(key):
        remote[key] = reduce_next(remote[key], 1, 0)

    def group_remote(key):
        group = cuts[key[1]][0]
        remote[key] = reduce_whole(remote[key], 1 << top, off_group(group))

    def far_remote(key):
        group = cuts[key[1]][0]
        for b in range(low_bits, dp_bits):
            remote[key] = reduce_whole(remote[key], 1 << b, at_group(group))

    def far_own(state):
        for b in range(low_bits, dp_bits):
            state = reduce_whole(state, 1 << b)
        return state

    def of(k):
        return [key for key in keys if key[1] == k]

    last = len(cuts) - 1
    for key in of(0):
        begin_remote(key)
    for key in of(0):
        next_remote(key)
    state = reduce_next(state, top, 0)
    if last > 1:
        for key in of(1):
            begin_remote(key)
        for key in of(1):
            next_remote(key)
    for key in of(0):
        group_remote(key)
    state = far_own(state)
    if last > 1:
        for key in of(1):
            group_remote(key)
    for key in of(last):
        begin_remote(key)
    for key in of(last):
        next_remote(key)
    for key in of(0):
        far_remote(key)
    if last > 1:
        for key in of(1):
            far_remote(key)
    for key in of(last):
        group_remote(key)

    sums, held = {}, {}
    sums["own"], pair = spread_first(state, None)
    held["own"] = pair
    for key in of(0):
        sums[key], held[key] = spread_first(remote[key], cuts[0][0])
    for key in of(last):
        far_remote(key)
    if last > 1:
        for key in of(1):
            sums[key], held[key] = spread_first(remote[key], cuts[1][0])

    def group_of(key):
        return None if key == "own" else cuts[key[1]][0]

    early = ["own"] + of(0)
    middle = of(1) if last > 1 else []
    for key in early:
        held[key] = spread_second(held[key], group_of(key))
    for key in early:
        held[key] = spread_third(*held[key])
    for key in of(last):
        sums[key], held[key] = spread_first(remote[key], cuts[last][0])
    for key in middle:
        held[key] = spread_second(held[key], group_of(key))
    for key in early:
        held[key] = spread_fourth(*held[key])
    for key in of(last):
        held[key] = spread_second(held[key], group_of(key))
    for key in middle:
        held[key] = spread_third(*held[key])

    grad_block = sums["own"]
    for r in range(1, count):
        groups = [[], []]
        for k, (group, start, stop) in enumerate(cuts):
            groups[group].append(sums[r, k])
        both = [parts[0] if len(parts) == 1 else jnp.concatenate(parts, 0) for parts in groups]
        grad_block = jnp.where(own == r, jnp.where(bit[top] == 0, both[0], both[1]), grad_block)
    grad_block = event(lambda g: g, grad_block)
    grad_high = grad_block.astype(BF16)
    grad_parts = [grad_high] + [swap(grad_high, "tensor", s) for s in range(1, count)]

    for key in of(last):
        held[key] = spread_third(*held[key])
    for key in middle:
        held[key] = spread_fourth(*held[key])
    for key in of(last):
        held[key] = spread_fourth(*held[key])

    right_rows = join(right_held, right_other, bit[0], dp_bits - 1).reshape(order, cols)

    arrays, where = [], {}
    for key in ["own"] + keys:
        for core in range(2):
            array = held[key][core]
            where[key, core] = len(arrays)
            arrays.append(array.reshape(count, -1, *array.shape[-2:]))
    runs, base, offset = [], [], 0
    for r in range(count):
        for core in range(2):
            for k, (group, start, stop) in enumerate(cuts):
                blocks = half // 2
                sources = []
                for s in range(count):
                    if r == s:
                        spot = (where["own", core], slice(group * blocks, (group + 1) * blocks), slice(start, stop))
                    else:
                        spot = (where[(r ^ s, k), core], slice(0, blocks), slice(0, stop - start))
                    sources.append(spot)
                length = blocks * (stop - start)
                runs.append((offset, length, sources))
                offset += length

    def in_order(natural):
        shape = natural.shape[:-1]
        blocks = natural.reshape(*shape, half, 2, rows)
        first = jnp.where(bit[0] == 0, blocks[..., 0, :], blocks[..., 1, :])
        second = jnp.where(bit[0] == 0, blocks[..., 1, :], blocks[..., 0, :])
        out = []
        for part in (first, second):
            for group, start, stop in cuts:
                out.append(part[..., group * (half // 2) : (group + 1) * (half // 2), start:stop].reshape(*shape, -1))
        return jnp.concatenate(out, -1)

    def from_order(mixed):
        at, sides = 0, []
        for core in range(2):
            groups = [[], []]
            for group, start, stop in cuts:
                length = half // 2 * (stop - start)
                groups[group].append(mixed[:, at : at + length].reshape(rows, half // 2, stop - start))
                at += length
            sides.append(jnp.concatenate([jnp.concatenate(parts, -1) for parts in groups], 1))
        first = jnp.where(bit[0] == 0, sides[0], sides[1])
        second = jnp.where(bit[0] == 0, sides[1], sides[0])
        return jnp.stack([first, second], 2).reshape(rows, cols)

    left_rows = jnp.concatenate([in_order(part) for part in left_parts], -1)
    span = jnp.arange(cols, dtype=jnp.int32)[None]
    positions = jnp.concatenate([in_order(span + r * cols) for r in range(count)], -1)
    positions = jnp.broadcast_to(positions, (8, order))
    scalars = jnp.stack([own * cols + low_place * rows, own, low_place * rows]).astype(jnp.int32)
    left_mixed, right_new, x, y, z, total = products(
        runs, count, scalars, left_rows, positions, right_rows, right_stat, grad_parts[1:], grad_block, arrays
    )
    masks = [("dp", 1 << b) for b in range(dp_bits)] + [("tensor", 1 << b) for b in range(tensor_bits)]
    other = swap(total, *masks[0])
    for mask in masks[1:]:
        total = total + other
        other = swap(total, *mask)
    left_new = from_order(left_mixed)
    update = finish(order, total, other, grad_block, x, y, z)
    return (left_new, right_new, update)


def solution(mesh):
    return jax.shard_map(
        local,
        mesh=mesh,
        in_specs=(P("dp", "tensor"),) * 4,
        out_specs=(P("dp", "tensor"),) * 3,
        check_vma=False,
    )
```

```python
import functools

import jax
import jax.numpy as jnp
import numpy as np
from jax import lax
from jax.experimental import pallas as pl
from jax.experimental.pallas import tpu as pltpu
from jax.sharding import PartitionSpec as P

BF16, F32 = jnp.bfloat16, jnp.float32
VMEM = pl.BlockSpec(memory_space=pltpu.VMEM)
SMEM = pl.BlockSpec(memory_space=pltpu.SMEM)


def exchange(x, axis, mask, sources=None):
    count = lax.axis_size(axis)
    pairs = [(i, i ^ mask) for i in range(count) if sources is None or sources(i)]
    return lax.ppermute(x, axis, pairs)


def dot(a, b, left, right):
    return lax.dot_general(a, b, (((left,), (right,)), ((), ())), preferred_element_type=F32)


def gram(features, others, core, rows):
    tokens, width = features.shape
    cols = others.shape[1]
    blocks = width // (2 * rows)
    shape = jax.ShapeDtypeStruct((blocks, rows, cols), F32)
    if rows % 128:
        total = dot(features, others, 0, 0).reshape(blocks, 2, rows, cols)
        pick = functools.partial(lax.dynamic_index_in_dim, total, axis=1, keepdims=False)
        return pick(core), pick(1 - core)

    def kernel(core_ref, a_ref, b_ref, keep_ref, send_ref):
        total = dot(a_ref[...], b_ref[...], 0, 0)
        first, second = total[:rows], total[rows:]
        keep_ref[0] = jnp.where(core_ref[0] == 0, first, second)
        send_ref[0] = jnp.where(core_ref[0] == 0, second, first)

    out = pl.BlockSpec((1, rows, cols), lambda i: (i, 0, 0))
    return pl.pallas_call(
        kernel,
        out_shape=(shape, shape),
        grid=(blocks,),
        in_specs=[SMEM, pl.BlockSpec((tokens, 2 * rows), lambda i: (0, i)), pl.BlockSpec((tokens, cols), lambda i: (0, 0))],
        out_specs=(out, out),
        compiler_params=pltpu.CompilerParams(vmem_limit_bytes=32 * 1024 * 1024),
        cost_estimate=pl.CostEstimate(flops=2 * tokens * width * cols, bytes_accessed=2 * tokens * (width + cols) + 4 * width * cols, transcendentals=0),
        name="gram",
    )(core.reshape(1), features, others)


def products(runs, count, scalars, left_parts, left_rows, positions, right_parts, right_stat, grad_parts, grad_block, arrays):
    rows, cols = grad_block.shape
    order = cols * count
    half = cols // 2
    tile = min(half, 256)
    low = cols // rows
    natural = left_rows is None

    def kernel(s_ref, pos_ref, stat_ref, grad_ref, *rest):
        left_refs, rest = rest[:count], rest[count:]
        right_refs, rest = rest[:2], rest[2:]
        grow_refs, rest = rest[: count - 1], rest[count - 1 :]
        refs, rest = rest[: len(arrays)], rest[len(arrays) :]
        left_out, right_out, x_out, y_out, z_out, sums_out, lnew, lsplit, turn, lhs, right_ref = rest

        def load(run, s, side, span=slice(None)):
            index, top = run[3][s][side]
            at = (s, slice(None)) if side == 0 else (slice(None), s)
            at += () if top is None else (top ^ s_ref[3],)
            return refs[index][at + (slice(None), span)].reshape(run[1], -1)

        def place(run, i):
            return pl.multiple_of((run[2][0] | ((s_ref[2] ^ run[2][1 + i]) & 3)) * rows, rows)

        for part, ref in enumerate(right_refs):
            bits = ref.shape[0].bit_length() - 1
            for j in range(ref.shape[0]):
                block = part + sum(((j >> (bits - 1 - i)) & 1) << (1 + i) for i in range(bits))
                top = (s_ref[1] ^ (block // low)) * cols
                right_ref[pl.ds(pl.multiple_of(top + (s_ref[2] ^ (block % low)) * rows, rows), rows), :] = ref[j]
        grad = grad_ref[...]
        grad_high = grad.astype(BF16)
        grad_low = (grad - grad_high.astype(F32)).astype(BF16)
        lhs[:rows, :cols] = grad_high
        for s in range(1, count):
            lhs[:rows, s * cols : (s + 1) * cols] = grow_refs[s - 1][...]
        both = jnp.concatenate([grad_high, grad_low], 0)
        for run in runs:
            value = dot(both[:, :half], load(run, 0, 0), 1, 1) + dot(both[:, half:], load(run, 0, 1), 1, 1)
            value = value[:rows] + value[rows:]
            for s in range(1, count):
                value += dot(grow_refs[s - 1][:, :half], load(run, s, 0), 1, 1)
                value += dot(grow_refs[s - 1][:, half:], load(run, s, 1), 1, 1)
            span = slice(run[0], run[0] + run[1])
            turn[:rows, span] = value.astype(BF16)
            if natural:
                r = run[0] // cols
                old = jnp.concatenate([left_refs[r][:, pl.ds(place(run, i), rows)] for i in range(2)], 1)
            else:
                old = left_refs[0][:, span]
            new = 0.9 * old + 0.1 * value
            lnew[:, span] = new
            if run[0] < cols:
                if natural:
                    for i in range(2):
                        left_out[:, pl.ds(place(run, i), rows)] = new[:, i * rows : (i + 1) * rows]
                else:
                    left_out[:, span] = new
            high = new.astype(BF16)
            lsplit[:rows, span] = high
            lsplit[rows:, span] = (new - high.astype(F32)).astype(BF16)
        spot = s_ref[0] + lax.broadcasted_iota(jnp.int32, (rows, order), 0)
        diagonal = jnp.sum(jnp.where(pos_ref[0:1, :] == spot, lnew[...], 0.0), 1, keepdims=True)
        for s in range(count):
            for n in range(0, cols, tile):
                value = None
                for run in runs:
                    base = load(run, s, n // half, slice(n % half, n % half + tile))
                    term = dot(lsplit[:, run[0] : run[0] + run[1]], base, 1, 0)
                    value = term if value is None else value + term
                value = value[:rows] + value[rows:]
                if s == 0:
                    value += diagonal * grad_low[:, n : n + tile].astype(F32)
                    x_out[:, n : n + tile] = value
                high = value.astype(BF16)
                span = slice(s * cols + n, s * cols + n + tile)
                lhs[rows : 2 * rows, span] = high
                lhs[2 * rows :, span] = (value - high.astype(F32)).astype(BF16)
        for run in runs:
            value = None
            for s in range(count):
                for side in range(2):
                    term = dot(lhs[rows : 2 * rows, s * cols + side * half : s * cols + (side + 1) * half], load(run, s, side), 1, 1)
                    value = term if value is None else value + term
            turn[rows:, run[0] : run[0] + run[1]] = value.astype(BF16)
        strips = []
        for run in runs:
            strip = None
            for s in range(count):
                for side in range(2):
                    start = s_ref[2] * rows - side * half
                    inside = (start >= 0) & (start < half)
                    if natural:
                        part = load(run, s, side, pl.ds(pl.multiple_of(jnp.where(inside, start, 0), rows), rows))
                    else:
                        wide = (half, rows)
                        pick = lax.broadcasted_iota(jnp.int32, wide, 0) == start + lax.broadcasted_iota(jnp.int32, wide, 1)
                        part = dot(load(run, s, side), pick.astype(F32).astype(BF16), 1, 0).astype(BF16)
                    keep = ((s_ref[1] == s) & inside).astype(F32).astype(BF16)
                    strip = part * keep if strip is None else strip + part * keep
            strips.append(strip)
        for n in range(0, cols, tile):
            span = slice(n, n + tile)
            stat = dot(lhs[...], right_ref[:, span], 1, 0)
            stat_low = dot(grad_low, right_ref[:cols, span], 1, 0)
            moved, total = None, None
            for run, strip in zip(runs, strips):
                base = load(run, 0, n // half, slice(n % half, n % half + tile))
                term = dot(turn[:, run[0] : run[0] + run[1]], base, 1, 0)
                moved = term if moved is None else moved + term
                term = dot(strip, base, 0, 0)
                total = term if total is None else total + term
            y_out[:, span] = 0.9 * (stat[:rows] + stat_low) + 0.1 * moved[:rows]
            z_out[:, span] = 0.9 * (stat[rows : 2 * rows] + stat[2 * rows :]) + 0.1 * moved[rows:]
            right_out[:, span] = 0.9 * stat_ref[:, span] + 0.1 * total
        terms = (grad, x_out[...], y_out[...], z_out[...])
        left, right = left_out[...], right_out[...]
        values = [left * left, right * right] + [terms[i] * terms[j] for i in range(4) for j in range(i, 4)]
        lane = lax.broadcasted_iota(jnp.int32, (8, 128), 1)
        total = jnp.zeros((8, 128), F32)
        for k, value in enumerate(values):
            total = jnp.where(lane == k, jnp.sum(value), total)
        sums_out[...] = total

    block = jax.ShapeDtypeStruct((rows, cols), F32)
    flops = 2 * rows * order * (2 * order + 2 * order + order + 5 * cols)
    lefts = list(left_parts) if natural else [left_rows] + list(left_parts[1:])
    operands = [positions, right_stat, grad_block, *lefts, *right_parts, *grad_parts, *arrays]
    return pl.pallas_call(
        kernel,
        out_shape=(block,) * 5 + (jax.ShapeDtypeStruct((8, 128), F32),),
        in_specs=[SMEM] + [VMEM] * len(operands),
        out_specs=(VMEM,) * 6,
        scratch_shapes=[
            pltpu.VMEM((rows, order), F32),
            pltpu.VMEM((2 * rows, order), BF16),
            pltpu.VMEM((2 * rows, order), BF16),
            pltpu.VMEM((3 * rows, order), BF16),
            pltpu.VMEM((order, cols), BF16),
        ],
        compiler_params=pltpu.CompilerParams(vmem_limit_bytes=48 * 1024 * 1024),
        cost_estimate=pl.CostEstimate(flops=flops, bytes_accessed=16 * order * cols, transcendentals=0),
        name="products",
    )(scalars, *operands)


def finish(order, mine, other, grad, x, y, z):
    rows, cols = grad.shape

    def kernel(a_ref, b_ref, g_ref, x_ref, y_ref, z_ref, out_ref):
        total = a_ref[...] + b_ref[...]
        lane = lax.broadcasted_iota(jnp.int32, total.shape, 1)

        def value(k):
            return jnp.sum(jnp.where(lane == k, total, 0.0), 1, keepdims=True)[0:1]

        left = 1.0 / jnp.sqrt(value(0) / order + 1e-06)
        right = 1.0 / jnp.sqrt(value(1) / order + 1e-06)
        weights = (jnp.full_like(left, 25.0), -5.0 * left, -5.0 * right, left * right)
        pairs = [(i, j) for i in range(4) for j in range(i, 4)]
        norm = 0.0
        for k, (i, j) in enumerate(pairs):
            norm = norm + (1.0 if i == j else 2.0) * weights[i] * weights[j] * value(2 + k)
        factor = jnp.sqrt(value(2) + 1e-06) / jnp.sqrt(jnp.maximum(norm, 0.0) + 1e-06)
        c0, c1, c2, c3 = [w * factor for w in weights]
        out_ref[...] = c0 * g_ref[...] + c1 * x_ref[...] + c2 * y_ref[...] + c3 * z_ref[...]

    return pl.pallas_call(
        kernel,
        out_shape=jax.ShapeDtypeStruct((rows, cols), F32),
        cost_estimate=pl.CostEstimate(flops=8 * rows * cols, bytes_accessed=20 * rows * cols, transcendentals=0),
        name="finish",
    )(mine, other, grad, x, y, z)


def local(activations, out_grads, left_stat, right_stat):
    count = lax.axis_size("tensor")
    dp_count = lax.axis_size("dp")
    tensor_bits = count.bit_length() - 1
    dp_bits = dp_count.bit_length() - 1
    low_bits = dp_bits - tensor_bits
    if low_bits != 3:
        raise ValueError(low_bits)
    low = 1 << low_bits
    _, cols = out_grads.shape
    order = cols * count
    rows = order // dp_count
    half = cols // 2
    place = lax.axis_index("dp")
    side = lax.axis_index("tensor")
    bit = [(place >> b) & 1 for b in range(dp_bits)]
    low_place = place & (low - 1)
    own = (place >> low_bits) ^ side
    top = low_bits - 1
    token = [None]

    def event(function, *inputs):
        if token[0] is not None:
            inputs, _ = lax.optimization_barrier((inputs, token[0]))
        out = function(*inputs)
        token[0] = out
        return out

    def at_group(group):
        return None if group is None else lambda i: ((i >> top) & 1) == group

    def off_group(group):
        return lambda i: ((i >> top) & 1) != group

    class Piece:
        def __init__(self, group):
            self.group = group

        def begin(self, features, others):
            self.keep, send = event(lambda f: gram(f, others, bit[0], rows), features)
            self.other = exchange(send, "dp", 1)

        def along_y(self):
            def step(k, r):
                k, r = [v.reshape(-1, 2, rows, v.shape[-1]) for v in (k, r)]
                take = functools.partial(lax.dynamic_index_in_dim, axis=1, keepdims=False)
                return take(k, bit[1]) + take(r, bit[1]), take(k, 1 - bit[1]) + take(r, 1 - bit[1])

            self.keep, send = event(step, self.keep, self.other)
            self.other = exchange(send, "dp", 2)

        def along_top(self):
            def step(k, r):
                take = functools.partial(lax.dynamic_index_in_dim, axis=0, keepdims=False)
                return take(k, bit[top]) + take(r, bit[top]), take(k, 1 - bit[top]) + take(r, 1 - bit[top])

            def whole(k, r):
                return (k + r)[0]

            if self.group is None:
                self.keep, send = event(step, self.keep, self.other)
                self.other = exchange(send, "dp", 1 << top)
            else:
                self.keep = event(whole, self.keep, self.other)
                self.other = exchange(self.keep, "dp", 1 << top, off_group(self.group))

        def far(self):
            for b in range(low_bits, dp_bits):
                self.keep = event(lambda k, r: k + r, self.keep, self.other)
                self.other = exchange(self.keep, "dp", 1 << b, at_group(self.group))

        def summed(self):
            def step(k, r):
                return k + r, (k + r).astype(BF16)

            self.sum, self.held = event(step, self.keep, self.other)
            self.other = exchange(self.held, "dp", 1 << top, at_group(self.group))

        def cut(self):
            group, width = self.group, self.held.shape[-1]

            def step(mine, other):
                if group is None:
                    held = jnp.stack([mine, other])
                else:
                    held = jnp.where(bit[top] == group, mine, other)
                return tuple(held[..., n : n + half] for n in range(0, width, half))

            return event(step, self.held, self.other)

    def y_first(held):
        return held, exchange(held, "dp", 2)

    def x_first(held):
        return held, [exchange(held, "tensor", s) for s in range(1, count)]

    def y_then_x(state):
        held = event(lambda m, o: jnp.stack([m, o]), *state)
        return held, [exchange(held, "tensor", s) for s in range(1, count)]

    def x_then_y(state):
        held = event(lambda m, o: jnp.stack([m] + o), *state)
        return held, exchange(held, "dp", 2)

    def x_last(state):
        held = event(lambda m, o: jnp.stack([m] + o), *state)
        return held, exchange(held, "dp", 1)

    def y_last(state):
        held = event(lambda m, o: jnp.stack([m, o]), *state)
        return held, exchange(held, "dp", 1)

    def send_features(group):
        width = cols // 2
        piece = event(lambda a: a[:, group * width : (group + 1) * width], activations)
        return [None] + [exchange(piece, "tensor", r) for r in range(1, count)]

    arrivals = [send_features(0)]
    right_held = event(lambda r: r.astype(BF16), right_stat)
    right_masks = [1 << b for b in range(dp_bits - 1, -1, -1)]
    right_other = exchange(right_held, "dp", right_masks[0])

    def right_next(held, other, level):
        held = event(lambda m, o: jnp.stack([m, o]), held, other)
        return held, exchange(held, "dp", right_masks[level + 1])

    arrivals.append(send_features(1))
    left_parts = [left_stat] + [exchange(left_stat, "tensor", s) for s in range(1, count)]

    mine = Piece(None)
    mine.begin(activations, out_grads)
    for level in range(dp_bits - 3):
        right_held, right_other = right_next(right_held, right_other, level)
    mine.along_y()
    shards = range(1, count)
    early = {r: Piece(0) for r in shards}
    late = {(r, side_): Piece(1) for r in shards for side_ in range(2)}
    lates = [[late[r, side_] for r in shards] for side_ in range(2)]
    for r in shards:
        early[r].begin(arrivals[0][r], out_grads)
    mine.along_top()
    for r in shards:
        early[r].along_y()
    right_held, right_other = right_next(right_held, right_other, dp_bits - 3)
    mine.far()
    for r in shards:
        early[r].along_top()
    for side_ in range(2):
        for r in shards:
            late[r, side_].begin(arrivals[1][r], out_grads[:, side_ * half : (side_ + 1) * half])
    for piece in lates[0]:
        piece.along_y()
    for r in shards:
        early[r].far()
    for piece in lates[1]:
        piece.along_y()
    mine.summed()
    for piece in lates[0]:
        piece.along_top()
    right_held, right_other = right_next(right_held, right_other, dp_bits - 2)
    ahead, behind = mine.cut()
    own_states = [y_first(ahead), x_first(behind)]
    for piece in lates[1]:
        piece.along_top()
    for r in shards:
        early[r].summed()
    for piece in lates[0]:
        piece.far()
    own_states = [y_then_x(own_states[0]), x_then_y(own_states[1])]
    for piece in lates[1]:
        piece.far()
    early_states = {}
    for r in shards:
        ahead, behind = early[r].cut()
        early_states[r] = [y_first(ahead), x_first(behind)]
    for piece in lates[0]:
        piece.summed()
    for piece in lates[1]:
        piece.summed()

    def own_rows(first, *others):
        block = first
        for r in shards:
            group0, left_half, right_half = others[3 * (r - 1) : 3 * r]
            group1 = jnp.concatenate([left_half, right_half], -1)
            block = jnp.where(own == r, jnp.where(bit[top] == 0, group0, group1), block)
        return block, block.astype(BF16)

    late_states = {}
    for r in shards:
        late_states[r, 0] = y_first(late[r, 0].cut()[0])
    own_states = [x_last(own_states[0]), y_last(own_states[1])]
    for r in shards:
        early_states[r] = [y_then_x(early_states[r][0]), x_then_y(early_states[r][1])]
    for r in shards:
        late_states[r, 1] = x_first(late[r, 1].cut()[0])
    for r in shards:
        late_states[r, 0] = y_then_x(late_states[r, 0])
    inputs = [v for r in shards for v in (early[r].sum, late[r, 0].sum, late[r, 1].sum)]
    grad_block, grad_high = event(own_rows, mine.sum, *inputs)
    grad_parts = [exchange(grad_high, "tensor", s) for s in range(1, count)]
    for r in shards:
        late_states[r, 1] = x_then_y(late_states[r, 1])
    for r in shards:
        early_states[r] = [x_last(early_states[r][0]), y_last(early_states[r][1])]
    for r in shards:
        late_states[r, 0] = x_last(late_states[r, 0])
    for r in shards:
        late_states[r, 1] = y_last(late_states[r, 1])

    arrays, where = [], {}
    for key, states in [("own", own_states)] + [((r, 0), early_states[r]) for r in shards] + [((r, 1), [late_states[r, 0], late_states[r, 1]]) for r in shards]:
        for side_, state in enumerate(states):
            for core, array in enumerate(state):
                where[key, side_, core] = len(arrays)
                arrays.append(array)
    runs, offset = [], 0
    length = 2 * rows
    for r in range(count):
        for group in range(2):
            for core in range(2):
                sources = []
                for s in range(count):
                    key = "own" if r == s else (r ^ s, group)
                    sources.append([(where[key, side_, core], group if r == s else None) for side_ in range(2)])
                runs.append((offset, length, (4 * group, core, 2 + core), sources))
                offset += length

    base = np.zeros((order,), np.int32)
    flips = np.zeros((2, order), np.int32)
    at = 0
    for r in range(count):
        for group in range(2):
            for core in range(2):
                for y in range(2):
                    base[at : at + rows] = r * cols + group * 4 * rows + np.arange(rows)
                    flips[0, at : at + rows] = core
                    flips[1, at : at + rows] = y
                    at += rows
    positions = base + rows * (flips[0] ^ bit[0]) + 2 * rows * (flips[1] ^ bit[1])
    positions = jnp.broadcast_to(positions[None], (8, order)).astype(jnp.int32)
    left_rows = None
    if rows % 128:
        left_rows = jnp.take(jnp.concatenate(left_parts, 1), positions[0], axis=1)
    scalars = jnp.stack([own * cols + low_place * rows, own, low_place, bit[top]]).astype(jnp.int32)
    right_parts = [v.reshape(-1, rows, cols) for v in (right_held, right_other)]
    left_new, right_new, x, y, z, total = products(
        runs, count, scalars, left_parts, left_rows, positions, right_parts, right_stat, grad_parts, grad_block, arrays
    )
    if rows % 128:
        left_new = jnp.zeros_like(left_new).at[:, positions[0, :cols]].set(left_new)
    masks = [("dp", 1 << b) for b in range(dp_bits)] + [("tensor", 1 << b) for b in range(tensor_bits)]
    other = exchange(total, *masks[0])
    for mask in masks[1:]:
        total = total + other
        other = exchange(total, *mask)
    update = finish(order, total, other, grad_block, x, y, z)
    return (left_new, right_new, update)


def solution(mesh):
    return jax.shard_map(
        local,
        mesh=mesh,
        in_specs=(P("dp", "tensor"),) * 4,
        out_specs=(P("dp", "tensor"),) * 3,
        check_vma=False,
    )
```

```python
import functools

import jax
import jax.numpy as jnp
import numpy as np
from jax import lax
from jax.experimental import pallas as pl
from jax.experimental.pallas import tpu as pltpu
from jax.sharding import PartitionSpec as P

BF16, F32 = jnp.bfloat16, jnp.float32
VMEM = pl.BlockSpec(memory_space=pltpu.VMEM)
SMEM = pl.BlockSpec(memory_space=pltpu.SMEM)


def exchange(x, axis, mask, sources=None):
    count = lax.axis_size(axis)
    pairs = [(i, i ^ mask) for i in range(count) if sources is None or sources(i)]
    return lax.ppermute(x, axis, pairs)


def dot(a, b, left, right):
    return lax.dot_general(a, b, (((left,), (right,)), ((), ())), preferred_element_type=F32)


def gram(features, others, core, rows, parts=1):
    tokens, width = features.shape
    cols = others.shape[1]
    blocks, part = width // (2 * rows), cols // parts
    shape = jax.ShapeDtypeStruct((blocks, rows, part), F32)
    if rows % 128:
        total = dot(features, others, 0, 0).reshape(blocks, 2, rows, parts, part)
        pick = functools.partial(lax.dynamic_index_in_dim, total, axis=1, keepdims=False)
        return [pick(c)[:, :, n] for c in (core, 1 - core) for n in range(parts)]

    def kernel(core_ref, a_ref, b_ref, *out_refs):
        for n in range(parts):
            total = dot(a_ref[...], b_ref[:, n * part : (n + 1) * part], 0, 0)
            first, second = total[:rows], total[rows:]
            out_refs[n][0] = jnp.where(core_ref[0] == 0, first, second)
            out_refs[parts + n][0] = jnp.where(core_ref[0] == 0, second, first)

    out = pl.BlockSpec((1, rows, part), lambda i: (i, 0, 0))
    return pl.pallas_call(
        kernel,
        out_shape=(shape,) * (2 * parts),
        grid=(blocks,),
        in_specs=[SMEM, pl.BlockSpec((tokens, 2 * rows), lambda i: (0, i)), pl.BlockSpec((tokens, cols), lambda i: (0, 0))],
        out_specs=(out,) * (2 * parts),
        compiler_params=pltpu.CompilerParams(vmem_limit_bytes=32 * 1024 * 1024),
        cost_estimate=pl.CostEstimate(flops=2 * tokens * width * cols, bytes_accessed=2 * tokens * (width + cols) + 4 * width * cols, transcendentals=0),
        name="gram",
    )(core.reshape(1), features, others)


def products(runs, count, scalars, left_parts, left_rows, positions, right_parts, right_stat, sums, arrays):
    rows, cols = right_stat.shape
    order = cols * count
    half = cols // 2
    tile = min(half, 256)
    low = cols // rows
    natural = left_rows is None

    def kernel(s_ref, pos_ref, stat_ref, *rest):
        left_refs, rest = rest[:count], rest[count:]
        right_refs, rest = rest[:4], rest[4:]
        sum_refs, rest = rest[: 2 * count], rest[2 * count :]
        refs, rest = rest[: len(arrays)], rest[len(arrays) :]
        left_out, right_out, grad_out, x_out, y_out, z_out, sums_out, lnew, lsplit, turn, lhs, right_ref = rest

        def load(run, s, side, span=slice(None)):
            ref = refs[run[3][s][side]]
            value = ref[s, :, :, :, span] if side == 0 else ref[:, s, :, :, span]
            return value.reshape(run[1], -1)

        def place(run, i):
            return pl.multiple_of((s_ref[2] ^ run[2][i]) * rows, rows)

        for number, ref in enumerate(right_refs):
            part, span = number % 2, slice(number // 2 * half, (number // 2 + 1) * half)
            bits = ref.shape[0].bit_length() - 1
            for j in range(ref.shape[0]):
                block = part + sum(((j >> (bits - 1 - i)) & 1) << (1 + i) for i in range(bits))
                top = (s_ref[1] ^ (block // low)) * cols
                right_ref[pl.ds(pl.multiple_of(top + (s_ref[2] ^ (block % low)) * rows, rows), rows), span] = ref[j]
        grad = None
        for r in range(count):
            part = jnp.concatenate([sum_refs[2 * r][...], sum_refs[2 * r + 1][...]], 1)
            grad = part if grad is None else jnp.where(s_ref[1] == r, part, grad)
        grad_out[...] = grad
        grad_high = grad.astype(BF16)
        grad_low = (grad - grad_high.astype(F32)).astype(BF16)
        lhs[:rows, :cols] = grad_high
        for s in range(1, count):
            for side in range(2):
                row = None
                for r in range(count):
                    ref = refs[runs[2 * r][3][s][side]]
                    part = ref[s, 0, 0] if side == 0 else ref[0, s, 0]
                    part = part * (s_ref[1] == r).astype(F32).astype(BF16)
                    row = part if row is None else row + part
                lhs[:rows, s * cols + side * half : s * cols + (side + 1) * half] = row
        both = jnp.concatenate([grad_high, grad_low], 0)
        for run in runs:
            value = dot(both[:, :half], load(run, 0, 0), 1, 1) + dot(both[:, half:], load(run, 0, 1), 1, 1)
            value = value[:rows] + value[rows:]
            for s in range(1, count):
                value += dot(lhs[:rows, s * cols : s * cols + half], load(run, s, 0), 1, 1)
                value += dot(lhs[:rows, s * cols + half : (s + 1) * cols], load(run, s, 1), 1, 1)
            span = slice(run[0], run[0] + run[1])
            turn[:rows, span] = value.astype(BF16)
            if natural:
                r = run[0] // cols
                old = jnp.concatenate([left_refs[r][:, pl.ds(place(run, i), rows)] for i in range(4)], 1)
            else:
                old = left_refs[0][:, span]
            new = 0.9 * old + 0.1 * value
            lnew[:, span] = new
            if run[0] < cols:
                if natural:
                    for i in range(4):
                        left_out[:, pl.ds(place(run, i), rows)] = new[:, i * rows : (i + 1) * rows]
                else:
                    left_out[:, span] = new
            high = new.astype(BF16)
            lsplit[:, span] = high
        spot = s_ref[0] + lax.broadcasted_iota(jnp.int32, (rows, order), 0)
        diagonal = jnp.sum(jnp.where(pos_ref[0:1, :] == spot, lnew[...], 0.0), 1, keepdims=True)
        diagonal_low = diagonal - diagonal.astype(BF16).astype(F32)
        for s in range(count):
            for n in range(0, cols, tile):
                value = None
                for run in runs:
                    base = load(run, s, n // half, slice(n % half, n % half + tile))
                    term = dot(lsplit[:, run[0] : run[0] + run[1]], base, 1, 0)
                    value = term if value is None else value + term
                span = slice(s * cols + n, s * cols + n + tile)
                value += diagonal_low * lhs[:rows, span].astype(F32)
                if s == 0:
                    value += diagonal * grad_low[:, n : n + tile].astype(F32)
                    x_out[:, n : n + tile] = value
                lhs[rows:, span] = value.astype(BF16)
        for run in runs:
            value = None
            for s in range(count):
                for side in range(2):
                    term = dot(lhs[rows:, s * cols + side * half : s * cols + (side + 1) * half], load(run, s, side), 1, 1)
                    value = term if value is None else value + term
            turn[rows:, run[0] : run[0] + run[1]] = value.astype(BF16)
        strips = []
        for run in runs:
            strip = None
            for s in range(count):
                for side in range(2):
                    start = s_ref[2] * rows - side * half
                    inside = (start >= 0) & (start < half)
                    if natural:
                        part = load(run, s, side, pl.ds(pl.multiple_of(jnp.where(inside, start, 0), rows), rows))
                    else:
                        wide = (half, rows)
                        pick = lax.broadcasted_iota(jnp.int32, wide, 0) == start + lax.broadcasted_iota(jnp.int32, wide, 1)
                        part = dot(load(run, s, side), pick.astype(F32).astype(BF16), 1, 0).astype(BF16)
                    keep = ((s_ref[1] == s) & inside).astype(F32).astype(BF16)
                    strip = part * keep if strip is None else strip + part * keep
            strips.append(strip)
        for n in range(0, cols, tile):
            span = slice(n, n + tile)
            stat = dot(lhs[...], right_ref[:, span], 1, 0)
            stat_low = dot(grad_low, right_ref[:cols, span], 1, 0)
            moved, total = None, None
            for run, strip in zip(runs, strips):
                base = load(run, 0, n // half, slice(n % half, n % half + tile))
                term = dot(turn[:, run[0] : run[0] + run[1]], base, 1, 0)
                moved = term if moved is None else moved + term
                term = dot(strip, base, 0, 0)
                total = term if total is None else total + term
            y_out[:, span] = 0.9 * (stat[:rows] + stat_low) + 0.1 * moved[:rows]
            z_out[:, span] = 0.9 * stat[rows:] + 0.1 * moved[rows:]
            right_out[:, span] = 0.9 * stat_ref[:, span] + 0.1 * total
        terms = (grad, x_out[...], y_out[...], z_out[...])
        left, right = left_out[...], right_out[...]
        values = [left * left, right * right] + [terms[i] * terms[j] for i in range(4) for j in range(i, 4)]
        lane = lax.broadcasted_iota(jnp.int32, (8, 128), 1)
        total = jnp.zeros((8, 128), F32)
        for k, value in enumerate(values):
            total = jnp.where(lane == k, jnp.sum(value), total)
        sums_out[...] = total

    block = jax.ShapeDtypeStruct((rows, cols), F32)
    flops = 2 * rows * order * (2 * order + 2 * order + order + 5 * cols)
    lefts = list(left_parts) if natural else [left_rows] + list(left_parts[1:])
    operands = [positions, right_stat, *lefts, *right_parts, *sums, *arrays]
    return pl.pallas_call(
        kernel,
        out_shape=(block,) * 6 + (jax.ShapeDtypeStruct((8, 128), F32),),
        in_specs=[SMEM] + [VMEM] * len(operands),
        out_specs=(VMEM,) * 7,
        scratch_shapes=[
            pltpu.VMEM((rows, order), F32),
            pltpu.VMEM((rows, order), BF16),
            pltpu.VMEM((2 * rows, order), BF16),
            pltpu.VMEM((2 * rows, order), BF16),
            pltpu.VMEM((order, cols), BF16),
        ],
        compiler_params=pltpu.CompilerParams(vmem_limit_bytes=48 * 1024 * 1024),
        cost_estimate=pl.CostEstimate(flops=flops, bytes_accessed=16 * order * cols, transcendentals=0),
        name="products",
    )(scalars, *operands)


def finish(order, mine, other, grad, x, y, z):
    rows, cols = grad.shape

    def kernel(a_ref, b_ref, g_ref, x_ref, y_ref, z_ref, out_ref):
        total = a_ref[...] + b_ref[...]
        lane = lax.broadcasted_iota(jnp.int32, total.shape, 1)

        def value(k):
            return jnp.sum(jnp.where(lane == k, total, 0.0), 1, keepdims=True)[0:1]

        left = 1.0 / jnp.sqrt(value(0) / order + 1e-06)
        right = 1.0 / jnp.sqrt(value(1) / order + 1e-06)
        weights = (jnp.full_like(left, 25.0), -5.0 * left, -5.0 * right, left * right)
        pairs = [(i, j) for i in range(4) for j in range(i, 4)]
        norm = 0.0
        for k, (i, j) in enumerate(pairs):
            norm = norm + (1.0 if i == j else 2.0) * weights[i] * weights[j] * value(2 + k)
        factor = jnp.sqrt(value(2) + 1e-06) / jnp.sqrt(jnp.maximum(norm, 0.0) + 1e-06)
        c0, c1, c2, c3 = [w * factor for w in weights]
        out_ref[...] = c0 * g_ref[...] + c1 * x_ref[...] + c2 * y_ref[...] + c3 * z_ref[...]

    return pl.pallas_call(
        kernel,
        out_shape=jax.ShapeDtypeStruct((rows, cols), F32),
        in_specs=[VMEM] * 6,
        out_specs=VMEM,
        cost_estimate=pl.CostEstimate(flops=8 * rows * cols, bytes_accessed=20 * rows * cols, transcendentals=0),
        name="finish",
    )(mine, other, grad, x, y, z)


def local(activations, out_grads, left_stat, right_stat):
    count = lax.axis_size("tensor")
    dp_count = lax.axis_size("dp")
    tensor_bits = count.bit_length() - 1
    dp_bits = dp_count.bit_length() - 1
    low_bits = dp_bits - tensor_bits
    if low_bits != 3:
        raise ValueError(low_bits)
    low = 1 << low_bits
    _, cols = out_grads.shape
    order = cols * count
    rows = order // dp_count
    half = cols // 2
    place = lax.axis_index("dp")
    side = lax.axis_index("tensor")
    bit = [(place >> b) & 1 for b in range(dp_bits)]
    low_place = place & (low - 1)
    own = (place >> low_bits) ^ side
    top = low_bits - 1
    token = [None]

    def event(function, *inputs):
        if token[0] is not None:
            inputs, _ = lax.optimization_barrier((inputs, token[0]))
        out = function(*inputs)
        token[0] = out
        return out

    def at_group(group):
        return None if group is None else lambda i: ((i >> top) & 1) == group

    def off_group(group):
        return lambda i: ((i >> top) & 1) != group

    class Piece:
        def __init__(self, group):
            self.group = group

        def begin(self, features, others):
            self.keep, send = event(lambda f: gram(f, others, bit[0], rows), features)
            self.other = exchange(send, "dp", 1)

        def along_y(self):
            def step(k, r):
                k, r = [v.reshape(-1, 2, rows, v.shape[-1]) for v in (k, r)]
                take = functools.partial(lax.dynamic_index_in_dim, axis=1, keepdims=False)
                return take(k, bit[1]) + take(r, bit[1]), take(k, 1 - bit[1]) + take(r, 1 - bit[1])

            self.keep, send = event(step, self.keep, self.other)
            self.other = exchange(send, "dp", 2)

        def along_top(self):
            def step(k, r):
                take = functools.partial(lax.dynamic_index_in_dim, axis=0, keepdims=False)
                return take(k, bit[top]) + take(r, bit[top]), take(k, 1 - bit[top]) + take(r, 1 - bit[top])

            def whole(k, r):
                return (k + r)[0]

            if self.group is None:
                self.keep, send = event(step, self.keep, self.other)
                self.other = exchange(send, "dp", 1 << top)
            else:
                self.keep = event(whole, self.keep, self.other)
                self.other = exchange(self.keep, "dp", 1 << top, off_group(self.group))

        def far(self):
            for b in range(low_bits, dp_bits):
                self.keep = event(lambda k, r: k + r, self.keep, self.other)
                self.other = exchange(self.keep, "dp", 1 << b, at_group(self.group))

        def summed(self):
            def step(k, r):
                return k + r, (k + r).astype(BF16)

            self.sum, self.held = event(step, self.keep, self.other)
            self.other = exchange(self.held, "dp", 1 << top, at_group(self.group))

        def cut(self):
            group, width = self.group, self.held.shape[-1]

            def step(mine, other):
                if group is None:
                    held = jnp.stack([mine, other])
                else:
                    held = jnp.where(bit[top] == group, mine, other)
                return tuple(held[..., n : n + half] for n in range(0, width, half))

            return event(step, self.held, self.other)

    def y_first(held):
        return held, exchange(held, "dp", 2)

    def x_first(held):
        return held, [exchange(held, "tensor", s) for s in range(1, count)]

    def y_then_x(state):
        held = event(lambda m, o: jnp.stack([m, o]), *state)
        return held, [exchange(held, "tensor", s) for s in range(1, count)]

    def x_then_y(state):
        held = event(lambda m, o: jnp.stack([m] + o), *state)
        return held, exchange(held, "dp", 2)

    def x_last(state):
        held = event(lambda m, o: jnp.stack([m] + o), *state)
        return held, exchange(held, "dp", 1)

    def y_last(state):
        held = event(lambda m, o: jnp.stack([m, o]), *state)
        return held, exchange(held, "dp", 1)

    def send_features(group):
        width = cols // 2
        piece = event(lambda a: a[:, group * width : (group + 1) * width], activations)
        return [None] + [exchange(piece, "tensor", r) for r in range(1, count)]

    arrivals = [send_features(0)]
    right_held = event(lambda r: r.astype(BF16), right_stat)
    right_masks = [1 << b for b in range(dp_bits - 1, 1, -1)]
    right_other = exchange(right_held, "dp", right_masks[0])
    owns = [Piece(None), Piece(None)]
    owns[0].keep, owns[1].keep, *sends = event(lambda f: gram(f, out_grads, bit[0], rows, 2), activations)
    owns[0].other, owns[1].other = [exchange(v, "dp", 1) for v in sends]
    arrivals.append(send_features(1))
    left_parts = [left_stat] + [exchange(left_stat, "tensor", s) for s in range(1, count)]

    def halve(piece, b, axis, shape):
        def step(k, r):
            k, r = [v.reshape(*shape, rows, half) for v in (k, r)]
            take = functools.partial(lax.dynamic_index_in_dim, axis=axis, keepdims=False)
            return take(k, bit[b]) + take(r, bit[b]), take(k, 1 - bit[b]) + take(r, 1 - bit[b])

        piece.keep, send = event(step, piece.keep, piece.other)
        piece.other = exchange(send, "dp", 1 << b)

    shards = range(1, count)
    early = {r: Piece(0) for r in shards}
    late = {(r, side_): Piece(1) for r in shards for side_ in range(2)}
    lates = [[late[r, side_] for r in shards] for side_ in range(2)]
    for mask in right_masks[1:]:
        right_held = event(lambda m, o: jnp.stack([m, o]), right_held, right_other)
        right_other = exchange(right_held, "dp", mask)
    halve(owns[0], 1, 1, (2, 2))
    halve(owns[1], top, 0, (2, 2))
    rights = event(lambda m, o: tuple(jnp.stack([m[..., n : n + half], o[..., n : n + half]]) for n in (0, half)), right_held, right_other)
    right_sides = [(rights[0], exchange(rights[0], "dp", 2))]
    halve(owns[0], top, 0, (2,))
    for r in shards:
        early[r].begin(arrivals[0][r], out_grads)
    halve(owns[1], 1, 0, (2,))
    for r in shards:
        early[r].along_y()
    right_sides.append((rights[1], exchange(rights[1], "dp", 2)))
    owns[0].far()
    owns[1].far()

    def right_last(number):
        held = event(lambda m, o: jnp.stack([m, o]), *right_sides[number])
        right_sides[number] = (held, exchange(held, "dp", 1))

    right_last(0)
    owns[0].summed()
    for r in shards:
        early[r].along_top()
    owns[1].summed()
    for side_ in range(2):
        for r in shards:
            late[r, side_].begin(arrivals[1][r], out_grads[:, side_ * half : (side_ + 1) * half])
    for piece in lates[0]:
        piece.along_y()
    for piece in lates[1]:
        piece.along_y()
    for r in shards:
        early[r].far()
    own_states = [None, x_first(*owns[1].cut())]
    for piece in lates[0]:
        piece.along_top()
    own_states[0] = y_first(*owns[0].cut())
    for piece in lates[1]:
        piece.along_top()
    own_states[1] = x_then_y(own_states[1])
    for piece in lates[0]:
        piece.far()
    right_last(1)
    for piece in lates[1]:
        piece.far()
    own_states[0] = y_then_x(own_states[0])
    whole = {}
    for side_ in range(2):
        for r in shards:

            def chosen(k, r_, ek, er, side_=side_):
                span = slice(side_ * half, (side_ + 1) * half)
                total = jnp.where(bit[top] == 0, ek[:, span] + er[:, span], k + r_)
                return total, total.astype(BF16)

            piece = whole[r, side_] = Piece(None)
            source = late[r, side_]
            piece.sum, piece.held = event(chosen, source.keep, source.other, early[r].keep, early[r].other)
            piece.other = exchange(piece.held, "dp", 1 << top)
    states = {}
    for r in shards:
        states[r, 0] = y_first(*whole[r, 0].cut())
    own_states[1] = y_last(own_states[1])
    for r in shards:
        states[r, 1] = x_first(*whole[r, 1].cut())
    own_states[0] = x_last(own_states[0])
    sums = [piece.sum for piece in owns] + [whole[r, side_].sum for r in shards for side_ in range(2)]
    for r in shards:
        states[r, 0] = y_then_x(states[r, 0])
    for r in shards:
        states[r, 1] = x_then_y(states[r, 1])
    for r in shards:
        states[r, 0] = x_last(states[r, 0])
    for r in shards:
        states[r, 1] = y_last(states[r, 1])

    arrays, where = [], {}
    for r in range(count):
        for side_ in range(2):
            state = own_states[side_] if r == 0 else states[r, side_]
            for core, array in enumerate(state):
                where[r, side_, core] = len(arrays)
                arrays.append(array)
    runs, offset = [], 0
    base = np.zeros((order,), np.int32)
    flips = np.zeros((order,), np.int32)
    for r in range(count):
        for core in range(2):
            blocks = [core | (y << 1) | (t << top) for y in range(2) for t in range(2)]
            sources = [[where[r ^ s, side_, core] for side_ in range(2)] for s in range(count)]
            runs.append((offset, 4 * rows, blocks, sources))
            for block in blocks:
                base[offset : offset + rows] = r * cols + np.arange(rows)
                flips[offset : offset + rows] = block
                offset += rows
    positions = base + rows * (flips ^ low_place)
    positions = jnp.broadcast_to(positions[None], (8, order)).astype(jnp.int32)
    left_rows = None
    if rows % 128:
        left_rows = jnp.take(jnp.concatenate(left_parts, 1), positions[0], axis=1)
    scalars = jnp.stack([own * cols + low_place * rows, own, low_place]).astype(jnp.int32)
    right_parts = [v.reshape(-1, rows, half) for state in right_sides for v in state]
    left_new, right_new, grad_block, x, y, z, total = products(
        runs, count, scalars, left_parts, left_rows, positions, right_parts, right_stat, sums, arrays
    )
    if rows % 128:
        left_new = jnp.zeros_like(left_new).at[:, positions[0, :cols]].set(left_new)
    masks = [("dp", 1 << b) for b in range(dp_bits)] + [("tensor", 1 << b) for b in range(tensor_bits)]
    other = exchange(total, *masks[0])
    for mask in masks[1:]:
        total = total + other
        other = exchange(total, *mask)
    update = finish(order, total, other, grad_block, x, y, z)
    return (left_new, right_new, update)


def solution(mesh):
    return jax.shard_map(
        local,
        mesh=mesh,
        in_specs=(P("dp", "tensor"),) * 4,
        out_specs=(P("dp", "tensor"),) * 3,
        check_vma=False,
    )
```

```python
import functools

import jax
import jax.numpy as jnp
import numpy as np
from jax import lax
from jax.experimental import pallas as pl
from jax.experimental.pallas import tpu as pltpu
from jax.sharding import PartitionSpec as P

BF16, F32 = jnp.bfloat16, jnp.float32
VMEM = pl.BlockSpec(memory_space=pltpu.VMEM)
SMEM = pl.BlockSpec(memory_space=pltpu.SMEM)


def exchange(x, axis, mask, sources=None):
    count = lax.axis_size(axis)
    pairs = [(i, i ^ mask) for i in range(count) if sources is None or sources(i)]
    return lax.ppermute(x, axis, pairs)


def dot(a, b, left, right):
    return lax.dot_general(a, b, (((left,), (right,)), ((), ())), preferred_element_type=F32)


def gram(features, others, core, rows, parts=1):
    tokens, width = features.shape
    cols = others.shape[1]
    blocks, part = width // (2 * rows), cols // parts
    shape = jax.ShapeDtypeStruct((blocks, rows, part), F32)
    if rows % 128:
        total = dot(features, others, 0, 0).reshape(blocks, 2, rows, parts, part)
        pick = functools.partial(lax.dynamic_index_in_dim, total, axis=1, keepdims=False)
        return [pick(c)[:, :, n] for c in (core, 1 - core) for n in range(parts)]

    def kernel(core_ref, a_ref, b_ref, *out_refs):
        for n in range(parts):
            total = dot(a_ref[...], b_ref[:, n * part : (n + 1) * part], 0, 0)
            first, second = total[:rows], total[rows:]
            out_refs[n][0] = jnp.where(core_ref[0] == 0, first, second)
            out_refs[parts + n][0] = jnp.where(core_ref[0] == 0, second, first)

    out = pl.BlockSpec((1, rows, part), lambda i: (i, 0, 0))
    return pl.pallas_call(
        kernel,
        out_shape=(shape,) * (2 * parts),
        grid=(blocks,),
        in_specs=[SMEM, pl.BlockSpec((tokens, 2 * rows), lambda i: (0, i)), pl.BlockSpec((tokens, cols), lambda i: (0, 0))],
        out_specs=(out,) * (2 * parts),
        compiler_params=pltpu.CompilerParams(vmem_limit_bytes=14 * 1024 * 1024),
        cost_estimate=pl.CostEstimate(flops=2 * tokens * width * cols, bytes_accessed=2 * tokens * (width + cols) + 4 * width * cols, transcendentals=0),
        name="gram",
    )(core.reshape(1), features, others)


def products(runs, count, scalars, left_parts, left_rows, positions, right_parts, right_stat, sums, arrays):
    rows, cols = right_stat.shape
    order = cols * count
    half = cols // 2
    tile = min(half, 256)
    low = cols // rows
    natural = left_rows is None

    def kernel(s_ref, pos_ref, stat_ref, *rest):
        left_refs, rest = rest[:count], rest[count:]
        right_refs, rest = rest[:4], rest[4:]
        sum_refs, rest = rest[: 2 * count], rest[2 * count :]
        refs, rest = rest[: len(arrays)], rest[len(arrays) :]
        left_out, right_out, grad_out, x_out, y_out, z_out, sums_out, lnew, lsplit, turn, lhs, right_ref = rest

        def load(run, s, side, span=slice(None)):
            ref = refs[run[3][s][side]]
            value = ref[s, :, :, :, span] if side == 0 else ref[:, s, :, :, span]
            return value.reshape(run[1], -1)

        def place(run, i):
            return pl.multiple_of((s_ref[2] ^ run[2][i]) * rows, rows)

        for number, ref in enumerate(right_refs):
            part, span = number % 2, slice(number // 2 * half, (number // 2 + 1) * half)
            bits = ref.shape[0].bit_length() - 1
            for j in range(ref.shape[0]):
                block = part + sum(((j >> (bits - 1 - i)) & 1) << (1 + i) for i in range(bits))
                top = (s_ref[1] ^ (block // low)) * cols
                right_ref[pl.ds(pl.multiple_of(top + (s_ref[2] ^ (block % low)) * rows, rows), rows), span] = ref[j]
        grad = None
        for r in range(count):
            part = jnp.concatenate([sum_refs[2 * r][...], sum_refs[2 * r + 1][...]], 1)
            grad = part if grad is None else jnp.where(s_ref[1] == r, part, grad)
        grad_out[...] = grad
        grad_high = grad.astype(BF16)
        grad_low = (grad - grad_high.astype(F32)).astype(BF16)
        lhs[:rows, :cols] = grad_high
        for s in range(1, count):
            for side in range(2):
                row = None
                for r in range(count):
                    ref = refs[runs[2 * r][3][s][side]]
                    part = ref[s, 0, 0] if side == 0 else ref[0, s, 0]
                    part = part * (s_ref[1] == r).astype(F32).astype(BF16)
                    row = part if row is None else row + part
                lhs[:rows, s * cols + side * half : s * cols + (side + 1) * half] = row
        both = jnp.concatenate([grad_high, grad_low], 0)
        for run in runs:
            value = dot(both[:, :half], load(run, 0, 0), 1, 1) + dot(both[:, half:], load(run, 0, 1), 1, 1)
            value = value[:rows] + value[rows:]
            for s in range(1, count):
                value += dot(lhs[:rows, s * cols : s * cols + half], load(run, s, 0), 1, 1)
                value += dot(lhs[:rows, s * cols + half : (s + 1) * cols], load(run, s, 1), 1, 1)
            span = slice(run[0], run[0] + run[1])
            turn[:rows, span] = value.astype(BF16)
            if natural:
                r = run[0] // cols
                old = jnp.concatenate([left_refs[r][:, pl.ds(place(run, i), rows)] for i in range(4)], 1)
            else:
                old = left_refs[0][:, span]
            new = 0.9 * old + 0.1 * value
            lnew[:, span] = new
            if run[0] < cols:
                if natural:
                    for i in range(4):
                        left_out[:, pl.ds(place(run, i), rows)] = new[:, i * rows : (i + 1) * rows]
                else:
                    left_out[:, span] = new
            high = new.astype(BF16)
            lsplit[:, span] = high
        spot = s_ref[0] + lax.broadcasted_iota(jnp.int32, (rows, order), 0)
        diagonal = jnp.sum(jnp.where(pos_ref[0:1, :] == spot, lnew[...], 0.0), 1, keepdims=True)
        diagonal_low = diagonal - diagonal.astype(BF16).astype(F32)
        for s in range(count):
            for n in range(0, cols, tile):
                value = None
                for run in runs:
                    base = load(run, s, n // half, slice(n % half, n % half + tile))
                    term = dot(lsplit[:, run[0] : run[0] + run[1]], base, 1, 0)
                    value = term if value is None else value + term
                span = slice(s * cols + n, s * cols + n + tile)
                value += diagonal_low * lhs[:rows, span].astype(F32)
                if s == 0:
                    value += diagonal * grad_low[:, n : n + tile].astype(F32)
                    x_out[:, n : n + tile] = value
                lhs[rows:, span] = value.astype(BF16)
        for run in runs:
            value = None
            for s in range(count):
                for side in range(2):
                    term = dot(lhs[rows:, s * cols + side * half : s * cols + (side + 1) * half], load(run, s, side), 1, 1)
                    value = term if value is None else value + term
            turn[rows:, run[0] : run[0] + run[1]] = value.astype(BF16)
        strips = []
        for run in runs:
            strip = None
            for s in range(count):
                for side in range(2):
                    start = s_ref[2] * rows - side * half
                    inside = (start >= 0) & (start < half)
                    if natural:
                        part = load(run, s, side, pl.ds(pl.multiple_of(jnp.where(inside, start, 0), rows), rows))
                    else:
                        wide = (half, rows)
                        pick = lax.broadcasted_iota(jnp.int32, wide, 0) == start + lax.broadcasted_iota(jnp.int32, wide, 1)
                        part = dot(load(run, s, side), pick.astype(F32).astype(BF16), 1, 0).astype(BF16)
                    keep = ((s_ref[1] == s) & inside).astype(F32).astype(BF16)
                    strip = part * keep if strip is None else strip + part * keep
            strips.append(strip)
        for n in range(0, cols, tile):
            span = slice(n, n + tile)
            stat = dot(lhs[...], right_ref[:, span], 1, 0)
            stat_low = dot(grad_low, right_ref[:cols, span], 1, 0)
            moved, total = None, None
            for run, strip in zip(runs, strips):
                base = load(run, 0, n // half, slice(n % half, n % half + tile))
                term = dot(turn[:, run[0] : run[0] + run[1]], base, 1, 0)
                moved = term if moved is None else moved + term
                term = dot(strip, base, 0, 0)
                total = term if total is None else total + term
            y_out[:, span] = 0.9 * (stat[:rows] + stat_low) + 0.1 * moved[:rows]
            z_out[:, span] = 0.9 * stat[rows:] + 0.1 * moved[rows:]
            right_out[:, span] = 0.9 * stat_ref[:, span] + 0.1 * total
        terms = (grad, x_out[...], y_out[...], z_out[...])
        left, right = left_out[...], right_out[...]
        values = [left * left, right * right] + [terms[i] * terms[j] for i in range(4) for j in range(i, 4)]
        lane = lax.broadcasted_iota(jnp.int32, (8, 128), 1)
        total = jnp.zeros((8, 128), F32)
        for k, value in enumerate(values):
            total = jnp.where(lane == k, jnp.sum(value), total)
        sums_out[...] = total

    block = jax.ShapeDtypeStruct((rows, cols), F32)
    flops = 2 * rows * order * (2 * order + 2 * order + order + 5 * cols)
    lefts = list(left_parts) if natural else [left_rows] + list(left_parts[1:])
    operands = [positions, right_stat, *lefts, *right_parts, *sums, *arrays]
    return pl.pallas_call(
        kernel,
        out_shape=(block,) * 6 + (jax.ShapeDtypeStruct((8, 128), F32),),
        in_specs=[SMEM] + [VMEM] * len(operands),
        out_specs=(VMEM,) * 7,
        scratch_shapes=[
            pltpu.VMEM((rows, order), F32),
            pltpu.VMEM((rows, order), BF16),
            pltpu.VMEM((2 * rows, order), BF16),
            pltpu.VMEM((2 * rows, order), BF16),
            pltpu.VMEM((order, cols), BF16),
        ],
        compiler_params=pltpu.CompilerParams(vmem_limit_bytes=26 * 1024 * 1024),
        cost_estimate=pl.CostEstimate(flops=flops, bytes_accessed=16 * order * cols, transcendentals=0),
        name="products",
    )(scalars, *operands)


def finish(order, mine, other, grad, x, y, z):
    rows, cols = grad.shape

    def kernel(a_ref, b_ref, g_ref, x_ref, y_ref, z_ref, out_ref):
        total = a_ref[...] + b_ref[...]
        lane = lax.broadcasted_iota(jnp.int32, total.shape, 1)

        def value(k):
            return jnp.sum(jnp.where(lane == k, total, 0.0), 1, keepdims=True)[0:1]

        left = 1.0 / jnp.sqrt(value(0) / order + 1e-06)
        right = 1.0 / jnp.sqrt(value(1) / order + 1e-06)
        weights = (jnp.full_like(left, 25.0), -5.0 * left, -5.0 * right, left * right)
        pairs = [(i, j) for i in range(4) for j in range(i, 4)]
        norm = 0.0
        for k, (i, j) in enumerate(pairs):
            norm = norm + (1.0 if i == j else 2.0) * weights[i] * weights[j] * value(2 + k)
        factor = jnp.sqrt(value(2) + 1e-06) / jnp.sqrt(jnp.maximum(norm, 0.0) + 1e-06)
        c0, c1, c2, c3 = [w * factor for w in weights]
        out_ref[...] = c0 * g_ref[...] + c1 * x_ref[...] + c2 * y_ref[...] + c3 * z_ref[...]

    return pl.pallas_call(
        kernel,
        out_shape=jax.ShapeDtypeStruct((rows, cols), F32),
        in_specs=[VMEM] * 6,
        out_specs=VMEM,
        compiler_params=pltpu.CompilerParams(vmem_limit_bytes=16 * rows * cols * 4),
        cost_estimate=pl.CostEstimate(flops=8 * rows * cols, bytes_accessed=20 * rows * cols, transcendentals=0),
        name="finish",
    )(mine, other, grad, x, y, z)


def local(activations, out_grads, left_stat, right_stat):
    count = lax.axis_size("tensor")
    dp_count = lax.axis_size("dp")
    tensor_bits = count.bit_length() - 1
    dp_bits = dp_count.bit_length() - 1
    low_bits = dp_bits - tensor_bits
    if low_bits != 3:
        raise ValueError(low_bits)
    low = 1 << low_bits
    _, cols = out_grads.shape
    order = cols * count
    rows = order // dp_count
    half = cols // 2
    place = lax.axis_index("dp")
    side = lax.axis_index("tensor")
    bit = [(place >> b) & 1 for b in range(dp_bits)]
    low_place = place & (low - 1)
    own = (place >> low_bits) ^ side
    top = low_bits - 1
    token = [None]

    def event(function, *inputs):
        if token[0] is not None:
            inputs, _ = lax.optimization_barrier((inputs, token[0]))
        out = function(*inputs)
        token[0] = out
        return out

    def at_group(group):
        return None if group is None else lambda i: ((i >> top) & 1) == group

    def off_group(group):
        return lambda i: ((i >> top) & 1) != group

    class Piece:
        def __init__(self, group):
            self.group = group

        def begin(self, features, others):
            self.keep, send = event(lambda f: gram(f, others, bit[0], rows), features)
            self.other = exchange(send, "dp", 1)

        def along_y(self):
            def step(k, r):
                k, r = [v.reshape(-1, 2, rows, v.shape[-1]) for v in (k, r)]
                take = functools.partial(lax.dynamic_index_in_dim, axis=1, keepdims=False)
                return take(k, bit[1]) + take(r, bit[1]), take(k, 1 - bit[1]) + take(r, 1 - bit[1])

            self.keep, send = event(step, self.keep, self.other)
            self.other = exchange(send, "dp", 2)

        def along_top(self):
            def step(k, r):
                take = functools.partial(lax.dynamic_index_in_dim, axis=0, keepdims=False)
                return take(k, bit[top]) + take(r, bit[top]), take(k, 1 - bit[top]) + take(r, 1 - bit[top])

            def whole(k, r):
                return (k + r)[0]

            if self.group is None:
                self.keep, send = event(step, self.keep, self.other)
                self.other = exchange(send, "dp", 1 << top)
            else:
                self.keep = event(whole, self.keep, self.other)
                self.other = exchange(self.keep, "dp", 1 << top, off_group(self.group))

        def far(self):
            for b in range(low_bits, dp_bits):
                self.keep = event(lambda k, r: k + r, self.keep, self.other)
                self.other = exchange(self.keep, "dp", 1 << b, at_group(self.group))

        def summed(self):
            def step(k, r):
                return k + r, (k + r).astype(BF16)

            self.sum, self.held = event(step, self.keep, self.other)
            self.other = exchange(self.held, "dp", 1 << top, at_group(self.group))

        def cut(self):
            group, width = self.group, self.held.shape[-1]

            def step(mine, other):
                if group is None:
                    held = jnp.stack([mine, other])
                else:
                    held = jnp.where(bit[top] == group, mine, other)
                return tuple(held[..., n : n + half] for n in range(0, width, half))

            return event(step, self.held, self.other)

    def y_first(held):
        return held, exchange(held, "dp", 2)

    def x_first(held):
        return held, [exchange(held, "tensor", s) for s in range(1, count)]

    def y_then_x(state):
        held = event(lambda m, o: jnp.stack([m, o]), *state)
        return held, [exchange(held, "tensor", s) for s in range(1, count)]

    def x_then_y(state):
        held = event(lambda m, o: jnp.stack([m] + o), *state)
        return held, exchange(held, "dp", 2)

    def x_last(state):
        held = event(lambda m, o: jnp.stack([m] + o), *state)
        return held, exchange(held, "dp", 1)

    def y_last(state):
        held = event(lambda m, o: jnp.stack([m, o]), *state)
        return held, exchange(held, "dp", 1)

    def send_features(group):
        width = cols // 2
        piece = event(lambda a: a[:, group * width : (group + 1) * width], activations)
        return [None] + [exchange(piece, "tensor", r) for r in range(1, count)]

    arrivals = [send_features(0)]
    right_held = event(lambda r: r.astype(BF16), right_stat)
    right_masks = [1 << b for b in range(dp_bits - 1, 1, -1)]
    right_other = exchange(right_held, "dp", right_masks[0])
    owns = [Piece(None), Piece(None)]
    owns[0].keep, owns[1].keep, *sends = event(lambda f: gram(f, out_grads, bit[0], rows, 2), activations)
    owns[0].other, owns[1].other = [exchange(v, "dp", 1) for v in sends]
    arrivals.append(send_features(1))
    left_parts = [left_stat] + [exchange(left_stat, "tensor", s) for s in range(1, count)]

    def halve(piece, b, axis, shape):
        def step(k, r):
            k, r = [v.reshape(*shape, rows, half) for v in (k, r)]
            take = functools.partial(lax.dynamic_index_in_dim, axis=axis, keepdims=False)
            return take(k, bit[b]) + take(r, bit[b]), take(k, 1 - bit[b]) + take(r, 1 - bit[b])

        piece.keep, send = event(step, piece.keep, piece.other)
        piece.other = exchange(send, "dp", 1 << b)

    shards = range(1, count)
    early = {r: Piece(0) for r in shards}
    late = {(r, side_): Piece(1) for r in shards for side_ in range(2)}
    lates = [[late[r, side_] for r in shards] for side_ in range(2)]
    for mask in right_masks[1:]:
        right_held = event(lambda m, o: jnp.stack([m, o]), right_held, right_other)
        right_other = exchange(right_held, "dp", mask)
    halve(owns[0], 1, 1, (2, 2))
    halve(owns[1], top, 0, (2, 2))
    rights = event(lambda m, o: tuple(jnp.stack([m[..., n : n + half], o[..., n : n + half]]) for n in (0, half)), right_held, right_other)
    right_sides = [(rights[0], exchange(rights[0], "dp", 2))]
    halve(owns[0], top, 0, (2,))
    for r in shards:
        early[r].begin(arrivals[0][r], out_grads)
    halve(owns[1], 1, 0, (2,))
    for r in shards:
        early[r].along_y()
    right_sides.append((rights[1], exchange(rights[1], "dp", 2)))
    owns[0].far()
    owns[1].far()

    def right_last(number):
        held = event(lambda m, o: jnp.stack([m, o]), *right_sides[number])
        right_sides[number] = (held, exchange(held, "dp", 1))

    right_last(0)
    owns[0].summed()
    for r in shards:
        early[r].along_top()
    owns[1].summed()
    for side_ in range(2):
        for r in shards:
            late[r, side_].begin(arrivals[1][r], out_grads[:, side_ * half : (side_ + 1) * half])
    for piece in lates[0]:
        piece.along_y()
    for piece in lates[1]:
        piece.along_y()
    for r in shards:
        early[r].far()
    own_states = [None, x_first(*owns[1].cut())]
    for piece in lates[0]:
        piece.along_top()
    own_states[0] = y_first(*owns[0].cut())
    for piece in lates[1]:
        piece.along_top()
    own_states[1] = x_then_y(own_states[1])
    for piece in lates[0]:
        piece.far()
    right_last(1)
    for piece in lates[1]:
        piece.far()
    own_states[0] = y_then_x(own_states[0])
    whole = {}
    for side_ in range(2):
        for r in shards:

            def chosen(k, r_, ek, er, side_=side_):
                span = slice(side_ * half, (side_ + 1) * half)
                total = jnp.where(bit[top] == 0, ek[:, span] + er[:, span], k + r_)
                return total, total.astype(BF16)

            piece = whole[r, side_] = Piece(None)
            source = late[r, side_]
            piece.sum, piece.held = event(chosen, source.keep, source.other, early[r].keep, early[r].other)
            piece.other = exchange(piece.held, "dp", 1 << top)
    states = {}
    for r in shards:
        states[r, 0] = y_first(*whole[r, 0].cut())
    own_states[1] = y_last(own_states[1])
    for r in shards:
        states[r, 1] = x_first(*whole[r, 1].cut())
    own_states[0] = x_last(own_states[0])
    sums = [piece.sum for piece in owns] + [whole[r, side_].sum for r in shards for side_ in range(2)]
    for r in shards:
        states[r, 0] = y_then_x(states[r, 0])
    for r in shards:
        states[r, 1] = x_then_y(states[r, 1])
    for r in shards:
        states[r, 0] = x_last(states[r, 0])
    for r in shards:
        states[r, 1] = y_last(states[r, 1])

    arrays, where = [], {}
    for r in range(count):
        for side_ in range(2):
            state = own_states[side_] if r == 0 else states[r, side_]
            for core, array in enumerate(state):
                where[r, side_, core] = len(arrays)
                arrays.append(array)
    runs, offset = [], 0
    base = np.zeros((order,), np.int32)
    flips = np.zeros((order,), np.int32)
    for r in range(count):
        for core in range(2):
            blocks = [core | (y << 1) | (t << top) for y in range(2) for t in range(2)]
            sources = [[where[r ^ s, side_, core] for side_ in range(2)] for s in range(count)]
            runs.append((offset, 4 * rows, blocks, sources))
            for block in blocks:
                base[offset : offset + rows] = r * cols + np.arange(rows)
                flips[offset : offset + rows] = block
                offset += rows
    positions = base + rows * (flips ^ low_place)
    positions = jnp.broadcast_to(positions[None], (8, order)).astype(jnp.int32)
    left_rows = None
    if rows % 128:
        left_rows = jnp.take(jnp.concatenate(left_parts, 1), positions[0], axis=1)
    scalars = jnp.stack([own * cols + low_place * rows, own, low_place]).astype(jnp.int32)
    right_parts = [v.reshape(-1, rows, half) for state in right_sides for v in state]
    left_new, right_new, grad_block, x, y, z, total = products(
        runs, count, scalars, left_parts, left_rows, positions, right_parts, right_stat, sums, arrays
    )
    if rows % 128:
        left_new = jnp.zeros_like(left_new).at[:, positions[0, :cols]].set(left_new)
    masks = [("dp", 1 << b) for b in range(dp_bits)] + [("tensor", 1 << b) for b in range(tensor_bits)]
    other = exchange(total, *masks[0])
    for mask in masks[1:]:
        total = total + other
        other = exchange(total, *mask)
    update = finish(order, total, other, grad_block, x, y, z)
    return (left_new, right_new, update)


def solution(mesh):
    return jax.shard_map(
        local,
        mesh=mesh,
        in_specs=(P("dp", "tensor"),) * 4,
        out_specs=(P("dp", "tensor"),) * 3,
        check_vma=False,
    )
```

```python
import functools

import jax
import jax.numpy as jnp
import numpy as np
from jax import lax
from jax.experimental import pallas as pl
from jax.experimental.pallas import tpu as pltpu
from jax.sharding import PartitionSpec as P

BF16, F32 = jnp.bfloat16, jnp.float32
VMEM = pl.BlockSpec(memory_space=pltpu.VMEM)
SMEM = pl.BlockSpec(memory_space=pltpu.SMEM)


def exchange(x, axis, mask, sources=None):
    count = lax.axis_size(axis)
    pairs = [(i, i ^ mask) for i in range(count) if sources is None or sources(i)]
    return lax.ppermute(x, axis, pairs)


def dot(a, b, left, right):
    return lax.dot_general(a, b, (((left,), (right,)), ((), ())), preferred_element_type=F32)


def gram(features, others, core, rows, parts=1):
    tokens, width = features.shape
    cols = others.shape[1]
    blocks, part = width // (2 * rows), cols // parts
    shape = jax.ShapeDtypeStruct((blocks, rows, part), F32)
    if rows % 128:
        total = dot(features, others, 0, 0).reshape(blocks, 2, rows, parts, part)
        pick = functools.partial(lax.dynamic_index_in_dim, total, axis=1, keepdims=False)
        return [pick(c)[:, :, n] for c in (core, 1 - core) for n in range(parts)]

    def kernel(core_ref, a_ref, b_ref, *out_refs):
        for n in range(parts):
            total = dot(a_ref[...], b_ref[:, n * part : (n + 1) * part], 0, 0)
            first, second = total[:rows], total[rows:]
            out_refs[n][0] = jnp.where(core_ref[0] == 0, first, second)
            out_refs[parts + n][0] = jnp.where(core_ref[0] == 0, second, first)

    out = pl.BlockSpec((1, rows, part), lambda i: (i, 0, 0))
    return pl.pallas_call(
        kernel,
        out_shape=(shape,) * (2 * parts),
        grid=(blocks,),
        in_specs=[SMEM, pl.BlockSpec((tokens, 2 * rows), lambda i: (0, i)), pl.BlockSpec((tokens, cols), lambda i: (0, 0))],
        out_specs=(out,) * (2 * parts),
        compiler_params=pltpu.CompilerParams(vmem_limit_bytes=14 * 1024 * 1024),
        cost_estimate=pl.CostEstimate(flops=2 * tokens * width * cols, bytes_accessed=2 * tokens * (width + cols) + 4 * width * cols, transcendentals=0),
        name="gram",
    )(core.reshape(1), features, others)


def products(runs, count, scalars, left_parts, left_rows, positions, right_parts, right_stat, sums, arrays):
    rows, cols = right_stat.shape
    order = cols * count
    half = cols // 2
    tile = min(half, 256)
    low = cols // rows
    natural = left_rows is None

    def kernel(s_ref, pos_ref, stat_ref, *rest):
        left_refs, rest = rest[:count], rest[count:]
        right_refs, rest = rest[:4], rest[4:]
        sum_refs, rest = rest[: 2 * count], rest[2 * count :]
        refs, rest = rest[: len(arrays)], rest[len(arrays) :]
        left_out, right_out, grad_out, x_out, y_out, z_out, sums_out, lnew, lsplit, turn, lhs, right_ref = rest

        def load(run, s, side, span=slice(None)):
            ref = refs[run[3][s][side]]
            value = ref[s, :, :, :, span] if side == 0 else ref[:, s, :, :, span]
            return value.reshape(run[1], -1)

        def place(run, i):
            return pl.multiple_of((s_ref[2] ^ run[2][i]) * rows, rows)

        for number, ref in enumerate(right_refs):
            part, span = number % 2, slice(number // 2 * half, (number // 2 + 1) * half)
            bits = ref.shape[0].bit_length() - 1
            for j in range(ref.shape[0]):
                block = part + sum(((j >> (bits - 1 - i)) & 1) << (1 + i) for i in range(bits))
                top = (s_ref[1] ^ (block // low)) * cols
                right_ref[pl.ds(pl.multiple_of(top + (s_ref[2] ^ (block % low)) * rows, rows), rows), span] = ref[j]
        grad = None
        for r in range(count):
            part = jnp.concatenate([sum_refs[2 * r][...], sum_refs[2 * r + 1][...]], 1)
            grad = part if grad is None else jnp.where(s_ref[1] == r, part, grad)
        grad_out[...] = grad
        grad_high = grad.astype(BF16)
        grad_low = (grad - grad_high.astype(F32)).astype(BF16)
        lhs[:rows, :cols] = grad_high
        for s in range(1, count):
            for side in range(2):
                row = None
                for r in range(count):
                    ref = refs[runs[2 * r][3][s][side]]
                    part = ref[s, 0, 0] if side == 0 else ref[0, s, 0]
                    part = part * (s_ref[1] == r).astype(F32).astype(BF16)
                    row = part if row is None else row + part
                lhs[:rows, s * cols + side * half : s * cols + (side + 1) * half] = row
        both = jnp.concatenate([grad_high, grad_low], 0)
        for run in runs:
            value = dot(both[:, :half], load(run, 0, 0), 1, 1) + dot(both[:, half:], load(run, 0, 1), 1, 1)
            value = value[:rows] + value[rows:]
            for s in range(1, count):
                value += dot(lhs[:rows, s * cols : s * cols + half], load(run, s, 0), 1, 1)
                value += dot(lhs[:rows, s * cols + half : (s + 1) * cols], load(run, s, 1), 1, 1)
            span = slice(run[0], run[0] + run[1])
            turn[:rows, span] = value.astype(BF16)
            if natural:
                r = run[0] // cols
                old = jnp.concatenate([left_refs[r][:, pl.ds(place(run, i), rows)] for i in range(4)], 1)
            else:
                old = left_refs[0][:, span]
            new = 0.9 * old + 0.1 * value
            lnew[:, span] = new
            if run[0] < cols:
                if natural:
                    for i in range(4):
                        left_out[:, pl.ds(place(run, i), rows)] = new[:, i * rows : (i + 1) * rows]
                else:
                    left_out[:, span] = new
            high = new.astype(BF16)
            lsplit[:, span] = high
        spot = s_ref[0] + lax.broadcasted_iota(jnp.int32, (rows, order), 0)
        diagonal = jnp.sum(jnp.where(pos_ref[0:1, :] == spot, lnew[...], 0.0), 1, keepdims=True)
        diagonal_low = diagonal - diagonal.astype(BF16).astype(F32)
        for s in range(count):
            for n in range(0, cols, tile):
                value = None
                for run in runs:
                    base = load(run, s, n // half, slice(n % half, n % half + tile))
                    term = dot(lsplit[:, run[0] : run[0] + run[1]], base, 1, 0)
                    value = term if value is None else value + term
                span = slice(s * cols + n, s * cols + n + tile)
                value += diagonal_low * lhs[:rows, span].astype(F32)
                if s == 0:
                    value += diagonal * grad_low[:, n : n + tile].astype(F32)
                    x_out[:, n : n + tile] = value
                lhs[rows:, span] = value.astype(BF16)
        for run in runs:
            value = None
            for s in range(count):
                for side in range(2):
                    term = dot(lhs[rows:, s * cols + side * half : s * cols + (side + 1) * half], load(run, s, side), 1, 1)
                    value = term if value is None else value + term
            turn[rows:, run[0] : run[0] + run[1]] = value.astype(BF16)
        strips = []
        for run in runs:
            strip = None
            for s in range(count):
                for side in range(2):
                    start = s_ref[2] * rows - side * half
                    inside = (start >= 0) & (start < half)
                    if natural:
                        part = load(run, s, side, pl.ds(pl.multiple_of(jnp.where(inside, start, 0), rows), rows))
                    else:
                        wide = (half, rows)
                        pick = lax.broadcasted_iota(jnp.int32, wide, 0) == start + lax.broadcasted_iota(jnp.int32, wide, 1)
                        part = dot(load(run, s, side), pick.astype(F32).astype(BF16), 1, 0).astype(BF16)
                    keep = ((s_ref[1] == s) & inside).astype(F32).astype(BF16)
                    strip = part * keep if strip is None else strip + part * keep
            strips.append(strip)
        for n in range(0, cols, tile):
            span = slice(n, n + tile)
            stat = dot(lhs[...], right_ref[:, span], 1, 0)
            stat_low = dot(grad_low, right_ref[:cols, span], 1, 0)
            moved, total = None, None
            for run, strip in zip(runs, strips):
                base = load(run, 0, n // half, slice(n % half, n % half + tile))
                term = dot(turn[:, run[0] : run[0] + run[1]], base, 1, 0)
                moved = term if moved is None else moved + term
                term = dot(strip, base, 0, 0)
                total = term if total is None else total + term
            y_out[:, span] = 0.9 * (stat[:rows] + stat_low) + 0.1 * moved[:rows]
            z_out[:, span] = 0.9 * stat[rows:] + 0.1 * moved[rows:]
            right_out[:, span] = 0.9 * stat_ref[:, span] + 0.1 * total
        terms = (grad, x_out[...], y_out[...], z_out[...])
        left, right = left_out[...], right_out[...]
        values = [left * left, right * right] + [terms[i] * terms[j] for i in range(4) for j in range(i, 4)]
        lane = lax.broadcasted_iota(jnp.int32, (8, 128), 1)
        total = jnp.zeros((8, 128), F32)
        for k, value in enumerate(values):
            total = jnp.where(lane == k, jnp.sum(value), total)
        sums_out[...] = total

    block = jax.ShapeDtypeStruct((rows, cols), F32)
    flops = 2 * rows * order * (2 * order + 2 * order + order + 5 * cols)
    lefts = list(left_parts) if natural else [left_rows] + list(left_parts[1:])
    operands = [positions, right_stat, *lefts, *right_parts, *sums, *arrays]
    return pl.pallas_call(
        kernel,
        out_shape=(block,) * 6 + (jax.ShapeDtypeStruct((8, 128), F32),),
        in_specs=[SMEM] + [VMEM] * len(operands),
        out_specs=(VMEM,) * 7,
        scratch_shapes=[
            pltpu.VMEM((rows, order), F32),
            pltpu.VMEM((rows, order), BF16),
            pltpu.VMEM((2 * rows, order), BF16),
            pltpu.VMEM((2 * rows, order), BF16),
            pltpu.VMEM((order, cols), BF16),
        ],
        compiler_params=pltpu.CompilerParams(vmem_limit_bytes=26 * 1024 * 1024),
        cost_estimate=pl.CostEstimate(flops=flops, bytes_accessed=16 * order * cols, transcendentals=0),
        name="products",
    )(scalars, *operands)


def finish(order, mine, other, grad, x, y, z):
    rows, cols = grad.shape

    def kernel(a_ref, b_ref, g_ref, x_ref, y_ref, z_ref, out_ref):
        total = a_ref[...] + b_ref[...]
        lane = lax.broadcasted_iota(jnp.int32, total.shape, 1)

        def value(k):
            return jnp.sum(jnp.where(lane == k, total, 0.0), 1, keepdims=True)[0:1]

        left = 1.0 / jnp.sqrt(value(0) / order + 1e-06)
        right = 1.0 / jnp.sqrt(value(1) / order + 1e-06)
        weights = (jnp.full_like(left, 25.0), -5.0 * left, -5.0 * right, left * right)
        pairs = [(i, j) for i in range(4) for j in range(i, 4)]
        norm = 0.0
        for k, (i, j) in enumerate(pairs):
            norm = norm + (1.0 if i == j else 2.0) * weights[i] * weights[j] * value(2 + k)
        factor = jnp.sqrt(value(2) + 1e-06) / jnp.sqrt(jnp.maximum(norm, 0.0) + 1e-06)
        c0, c1, c2, c3 = [w * factor for w in weights]
        out_ref[...] = c0 * g_ref[...] + c1 * x_ref[...] + c2 * y_ref[...] + c3 * z_ref[...]

    return pl.pallas_call(
        kernel,
        out_shape=jax.ShapeDtypeStruct((rows, cols), F32),
        in_specs=[VMEM] * 6,
        out_specs=VMEM,
        compiler_params=pltpu.CompilerParams(vmem_limit_bytes=16 * rows * cols * 4),
        cost_estimate=pl.CostEstimate(flops=8 * rows * cols, bytes_accessed=20 * rows * cols, transcendentals=0),
        name="finish",
    )(mine, other, grad, x, y, z)


def local(activations, out_grads, left_stat, right_stat):
    count = lax.axis_size("tensor")
    dp_count = lax.axis_size("dp")
    tensor_bits = count.bit_length() - 1
    dp_bits = dp_count.bit_length() - 1
    low_bits = dp_bits - tensor_bits
    if low_bits != 3:
        raise ValueError(low_bits)
    low = 1 << low_bits
    _, cols = out_grads.shape
    order = cols * count
    rows = order // dp_count
    half = cols // 2
    place = lax.axis_index("dp")
    side = lax.axis_index("tensor")
    bit = [(place >> b) & 1 for b in range(dp_bits)]
    low_place = place & (low - 1)
    own = (place >> low_bits) ^ side
    top = low_bits - 1
    token = [None]

    def event(function, *inputs):
        if token[0] is not None:
            inputs, _ = lax.optimization_barrier((inputs, token[0]))
        out = function(*inputs)
        token[0] = out
        return out

    def at_group(group):
        return None if group is None else lambda i: ((i >> top) & 1) == group

    def off_group(group):
        return lambda i: ((i >> top) & 1) != group

    class Piece:
        def __init__(self, group):
            self.group = group

        def begin(self, features, others):
            self.keep, send = event(lambda f: gram(f, others, bit[0], rows), features)
            self.other = exchange(send, "dp", 1)

        def along_y(self):
            def step(k, r):
                k, r = [v.reshape(-1, 2, rows, v.shape[-1]) for v in (k, r)]
                take = functools.partial(lax.dynamic_index_in_dim, axis=1, keepdims=False)
                return take(k, bit[1]) + take(r, bit[1]), take(k, 1 - bit[1]) + take(r, 1 - bit[1])

            self.keep, send = event(step, self.keep, self.other)
            self.other = exchange(send, "dp", 2)

        def along_top(self):
            def step(k, r):
                take = functools.partial(lax.dynamic_index_in_dim, axis=0, keepdims=False)
                return take(k, bit[top]) + take(r, bit[top]), take(k, 1 - bit[top]) + take(r, 1 - bit[top])

            def whole(k, r):
                return (k + r)[0]

            if self.group is None:
                self.keep, send = event(step, self.keep, self.other)
                self.other = exchange(send, "dp", 1 << top)
            else:
                self.keep = event(whole, self.keep, self.other)
                self.other = exchange(self.keep, "dp", 1 << top, off_group(self.group))

        def far(self):
            for b in range(low_bits, dp_bits):
                self.keep = event(lambda k, r: k + r, self.keep, self.other)
                self.other = exchange(self.keep, "dp", 1 << b, at_group(self.group))

        def summed(self):
            def step(k, r):
                return k + r, (k + r).astype(BF16)

            self.sum, self.held = event(step, self.keep, self.other)
            self.other = exchange(self.held, "dp", 1 << top, at_group(self.group))

        def cut(self):
            group, width = self.group, self.held.shape[-1]

            def step(mine, other):
                if group is None:
                    held = jnp.stack([mine, other])
                else:
                    held = jnp.where(bit[top] == group, mine, other)
                return tuple(held[..., n : n + half] for n in range(0, width, half))

            return event(step, self.held, self.other)

    def y_first(held):
        return held, exchange(held, "dp", 2)

    def x_first(held):
        return held, [exchange(held, "tensor", s) for s in range(1, count)]

    def y_then_x(state):
        held = event(lambda m, o: jnp.stack([m, o]), *state)
        return held, [exchange(held, "tensor", s) for s in range(1, count)]

    def x_then_y(state):
        held = event(lambda m, o: jnp.stack([m] + o), *state)
        return held, exchange(held, "dp", 2)

    def x_last(state):
        held = event(lambda m, o: jnp.stack([m] + o), *state)
        return held, exchange(held, "dp", 1)

    def y_last(state):
        held = event(lambda m, o: jnp.stack([m, o]), *state)
        return held, exchange(held, "dp", 1)

    def send_features(group):
        width = cols // 2
        piece = event(lambda a: a[:, group * width : (group + 1) * width], activations)
        return [None] + [exchange(piece, "tensor", r) for r in range(1, count)]

    arrivals = [send_features(0)]
    right_held = event(lambda r: r.astype(BF16), right_stat)
    right_masks = [1 << b for b in range(dp_bits - 1, 1, -1)]
    right_other = exchange(right_held, "dp", right_masks[0])
    owns = [Piece(None), Piece(None)]
    owns[0].keep, owns[1].keep, *sends = event(lambda f: gram(f, out_grads, bit[0], rows, 2), activations)
    owns[0].other, owns[1].other = [exchange(v, "dp", 1) for v in sends]
    arrivals.append(send_features(1))
    left_parts = [left_stat] + [exchange(left_stat, "tensor", s) for s in range(1, count)]

    def halve(piece, b, axis, shape):
        def step(k, r):
            k, r = [v.reshape(*shape, rows, half) for v in (k, r)]
            take = functools.partial(lax.dynamic_index_in_dim, axis=axis, keepdims=False)
            return take(k, bit[b]) + take(r, bit[b]), take(k, 1 - bit[b]) + take(r, 1 - bit[b])

        piece.keep, send = event(step, piece.keep, piece.other)
        piece.other = exchange(send, "dp", 1 << b)

    shards = range(1, count)
    early = {r: Piece(0) for r in shards}
    late = {(r, side_): Piece(1) for r in shards for side_ in range(2)}
    lates = [[late[r, side_] for r in shards] for side_ in range(2)]
    for mask in right_masks[1:]:
        right_held = event(lambda m, o: jnp.stack([m, o]), right_held, right_other)
        right_other = exchange(right_held, "dp", mask)
    halve(owns[0], 1, 1, (2, 2))
    halve(owns[1], top, 0, (2, 2))
    rights = event(lambda m, o: tuple(jnp.stack([m[..., n : n + half], o[..., n : n + half]]) for n in (0, half)), right_held, right_other)
    right_sides = [(rights[0], exchange(rights[0], "dp", 2))]
    halve(owns[0], top, 0, (2,))
    for r in shards:
        early[r].begin(arrivals[0][r], out_grads)
    halve(owns[1], 1, 0, (2,))
    for r in shards:
        early[r].along_y()
    right_sides.append((rights[1], exchange(rights[1], "dp", 2)))
    owns[0].far()
    owns[1].far()

    def right_last(number):
        held = event(lambda m, o: jnp.stack([m, o]), *right_sides[number])
        right_sides[number] = (held, exchange(held, "dp", 1))

    right_last(0)
    for r in shards:
        early[r].along_top()
    owns[0].summed()
    for side_ in range(2):
        for r in shards:
            late[r, side_].begin(arrivals[1][r], out_grads[:, side_ * half : (side_ + 1) * half])
    for piece in lates[0]:
        piece.along_y()
    for piece in lates[1]:
        piece.along_y()
    owns[1].summed()
    halves = {}

    def early_far(side_):
        span = slice(side_ * half, (side_ + 1) * half)
        for r in shards:
            piece = halves[r, side_] = Piece(0)
            piece.keep = event(lambda k, r_: k[:, span] + r_[:, span], early[r].keep, early[r].other)
            piece.other = exchange(piece.keep, "dp", 1 << low_bits, at_group(0))
            for b in range(low_bits + 1, dp_bits):
                piece.keep = event(lambda k, r_: k + r_, piece.keep, piece.other)
                piece.other = exchange(piece.keep, "dp", 1 << b, at_group(0))

    for piece in lates[0]:
        piece.along_top()
    early_far(0)
    for piece in lates[1]:
        piece.along_top()
    early_far(1)
    own_states = [y_first(*owns[0].cut()), None]
    for piece in lates[0]:
        piece.far()
    own_states[1] = x_first(*owns[1].cut())
    for piece in lates[1]:
        piece.far()
    own_states[0] = y_then_x(own_states[0])
    whole, states = {}, {}

    def choose(side_):
        def chosen(k, r_, ek, er):
            total = jnp.where(bit[top] == 0, ek + er, k + r_)
            return total, total.astype(BF16)

        for r in shards:
            piece = whole[r, side_] = Piece(None)
            first, second = halves[r, side_], late[r, side_]
            piece.sum, piece.held = event(chosen, second.keep, second.other, first.keep, first.other)
            piece.other = exchange(piece.held, "dp", 1 << top)

    choose(0)
    own_states[1] = x_then_y(own_states[1])
    choose(1)
    for r in shards:
        states[r, 0] = y_first(*whole[r, 0].cut())
    right_last(1)
    own_states[0] = x_last(own_states[0])
    for r in shards:
        states[r, 1] = x_first(*whole[r, 1].cut())
    own_states[1] = y_last(own_states[1])
    sums = [piece.sum for piece in owns] + [whole[r, side_].sum for r in shards for side_ in range(2)]
    for r in shards:
        states[r, 0] = y_then_x(states[r, 0])
    for r in shards:
        states[r, 1] = x_then_y(states[r, 1])
    for r in shards:
        states[r, 0] = x_last(states[r, 0])
    for r in shards:
        states[r, 1] = y_last(states[r, 1])

    arrays, where = [], {}
    for r in range(count):
        for side_ in range(2):
            state = own_states[side_] if r == 0 else states[r, side_]
            for core, array in enumerate(state):
                where[r, side_, core] = len(arrays)
                arrays.append(array)
    runs, offset = [], 0
    base = np.zeros((order,), np.int32)
    flips = np.zeros((order,), np.int32)
    for r in range(count):
        for core in range(2):
            blocks = [core | (y << 1) | (t << top) for y in range(2) for t in range(2)]
            sources = [[where[r ^ s, side_, core] for side_ in range(2)] for s in range(count)]
            runs.append((offset, 4 * rows, blocks, sources))
            for block in blocks:
                base[offset : offset + rows] = r * cols + np.arange(rows)
                flips[offset : offset + rows] = block
                offset += rows
    positions = base + rows * (flips ^ low_place)
    positions = jnp.broadcast_to(positions[None], (8, order)).astype(jnp.int32)
    left_rows = None
    if rows % 128:
        left_rows = jnp.take(jnp.concatenate(left_parts, 1), positions[0], axis=1)
    scalars = jnp.stack([own * cols + low_place * rows, own, low_place]).astype(jnp.int32)
    right_parts = [v.reshape(-1, rows, half) for state in right_sides for v in state]
    left_new, right_new, grad_block, x, y, z, total = products(
        runs, count, scalars, left_parts, left_rows, positions, right_parts, right_stat, sums, arrays
    )
    if rows % 128:
        left_new = jnp.zeros_like(left_new).at[:, positions[0, :cols]].set(left_new)
    masks = [("dp", 1 << b) for b in range(dp_bits)] + [("tensor", 1 << b) for b in range(tensor_bits)]
    other = exchange(total, *masks[0])
    for mask in masks[1:]:
        total = total + other
        other = exchange(total, *mask)
    update = finish(order, total, other, grad_block, x, y, z)
    return (left_new, right_new, update)


def solution(mesh):
    return jax.shard_map(
        local,
        mesh=mesh,
        in_specs=(P("dp", "tensor"),) * 4,
        out_specs=(P("dp", "tensor"),) * 3,
        check_vma=False,
    )
```
